256 devices in a mesh: section: 8 (over z_hi, x), dp: 32 (over y, z_lo, core).
Axes of the slice: x: 4, y: 4, z: 8 (z_hi: 2, z_lo: 4; z = z_hi * 4 + z_lo), core: 2. Of those that a mesh axis runs over, the one named last changes fastest.
Arguments:
- inputs: bfloat16 [4, 4096, 1536], P(None, 'dp'), may hold values from -6 to 6
- out_grad: bfloat16 [4, 4096, 1536], P(None, 'dp'), may hold values from -0.09375 to 0.09375
- guide_bin: int32 [4, 1], replicated, may hold values from 0 to 31
- time_step: int32 [4, 1], replicated, may hold values from 0 to 999
- guide_table: bfloat16 [32, 4608], replicated, may hold values from -3 to 3
- section_table: float32 [8, 3, 1536], P('section'), may hold values from -3 to 3
- value_weight: bfloat16 [8, 1536, 1536], P('section'), may hold values from -0.15625 to 0.15625
- proj_weight: bfloat16 [8, 1536, 1536], P('section'), may hold values from -0.15625 to 0.15625
Outputs:
- value_grad: float32 [8, 1536, 1536], P('section', 'dp')
- proj_grad: float32 [8, 1536, 1536], P('section', 'dp')
- table_grad: float32 [8, 3, 1536], P('section', None, 'dp')
The draws below stay inside these ranges and needn't reach their ends.
All inputs are finite; a program needn't handle non-finite values.
Results may differ from the reference program's by a relative error of at most 0.017.
Values may be sent and summed in bfloat16 or wider, within the bound.
No kernel may reach another device: no remote copies, remote signals or barrier semaphores. Data moves between devices by JAX's collectives and lax.ppermute only.
A program may use at most 128 MiB of HBM per device.

```python
import math
import jax
import jax.numpy as jnp
from jax import lax

D = 1536
H = 1536
MICRO = 4
BINS = 32
STEPS = 1000
TOKENS = 4096
SAMPLES = 1
BLOCKS = 8


def plant(drawn, own_key, least, high):
    dims = drawn.shape
    spot = [jax.random.randint(jax.random.fold_in(own_key, axis), (), 0, dims[axis]) for axis in range(len(dims))]
    drawn = drawn.at[tuple(spot)].set(least)
    longest = dims.index(max(dims))
    spot[longest] = (spot[longest] + 1) % dims[longest]
    return drawn.at[tuple(spot)].set(high)


def levels(key, extent, cuts, least, top_value):
    def one(axis_at, blocks):
        steps = jax.random.uniform(jax.random.fold_in(jax.random.fold_in(key, 6), axis_at), (blocks,), jnp.float32, least / len(cuts), top_value / len(cuts))
        return jnp.repeat(jnp.exp(steps), extent[axis_at] // blocks).reshape((-1,) + (1,) * (len(extent) - axis_at - 1))

    factor_of = one(*cuts[0])
    for cut in cuts[1:]:
        factor_of = factor_of * one(*cut)
    return factor_of


def normal_values(stream_key, extent, deviation, bound, pieces=(), kind=jnp.bfloat16):
    array = jax.random.normal(stream_key, extent, jnp.float32) * deviation
    if len(pieces) > 0:
        array = levels(stream_key, extent, pieces, -0.22, 0.18) * array
    return jnp.clip(array, min=-bound, max=bound).astype(kind)


def setup_inputs(seed: int = 0) -> dict:
    arg_keys = jax.random.split(jax.random.key(seed), 9)
    inputs = normal_values(arg_keys[0], (MICRO, TOKENS, D), 1.0, 6.0, ((1, 32),))
    out_grad = normal_values(arg_keys[1], (MICRO, TOKENS, D), TOKENS ** -0.5, 0.09375, ((1, 32),))
    guide_bin = plant(jax.random.randint(arg_keys[2], (MICRO, SAMPLES), 0, BINS), jax.random.fold_in(arg_keys[2], 1), 0, BINS - 1).astype(jnp.int32)
    time_step = plant(jax.random.randint(arg_keys[3], (MICRO, SAMPLES), 0, STEPS), jax.random.fold_in(arg_keys[3], 1), 0, STEPS - 1).astype(jnp.int32)
    guide_table = normal_values(arg_keys[4], (BINS, 3 * D), 0.5, 3.0)
    section_table = normal_values(arg_keys[5], (BLOCKS, 3, D), 0.5, 3.0, ((0, 8),), jnp.float32)
    value_weight = normal_values(arg_keys[6], (BLOCKS, D, H), D ** -0.5, 0.15625, ((0, 8),))
    proj_weight = normal_values(arg_keys[7], (BLOCKS, H, D), H ** -0.5, 0.15625, ((0, 8),))
    return {"inputs": inputs, "out_grad": out_grad, "guide_bin": guide_bin, "time_step": time_step, "guide_table": guide_table, "section_table": section_table, "value_weight": value_weight, "proj_weight": proj_weight}


NORM_FLOOR = 0.1

def normalize(hidden):
    centre = lax.optimization_barrier(jnp.mean(hidden, axis=-1, keepdims=True))
    centred = hidden - centre
    spread = lax.optimization_barrier(jnp.mean(centred * centred, axis=-1, keepdims=True))
    inverse = lax.rsqrt(spread + NORM_FLOOR)
    return (centred * inverse, inverse)

def conditions(guide_bin, time_step, guide_table):
    total = guide_table.shape[1]
    half = total // 2
    frequency = jnp.exp(-math.log(10000.0) * jnp.arange(half, dtype=jnp.float32) / half)
    angle = time_step.astype(jnp.float32)[..., None] * frequency
    waves = jnp.concatenate([jnp.sin(angle), jnp.cos(angle)], axis=-1)
    return guide_table.astype(jnp.float32)[guide_bin] + 0.5 * waves

def forward_block(block_in, modulation, value_weight, proj_weight):
    width = block_in.shape[1]
    hidden = block_in.astype(jnp.float32)
    normed, inverse = normalize(hidden)
    shift = modulation[:, :width]
    scale = modulation[:, width:2 * width]
    gate = modulation[:, 2 * width:]
    modulated = (normed * (1.0 + scale) + shift).astype(jnp.bfloat16)
    values = jnp.dot(modulated, value_weight, preferred_element_type=jnp.float32).astype(jnp.bfloat16)
    projected = jnp.dot(values, proj_weight, preferred_element_type=jnp.float32)
    block_out = (hidden + gate * projected).astype(jnp.bfloat16)
    return (block_out, modulated, values, projected)

def backward_block(block_in, modulated, values, projected, upstream, modulation, value_weight, proj_weight):
    width = block_in.shape[1]
    hidden = block_in.astype(jnp.float32)
    normed, inverse = normalize(hidden)
    scale = modulation[:, width:2 * width]
    gate = modulation[:, 2 * width:]
    grad_up = upstream.astype(jnp.float32)
    grad_proj = (gate * grad_up).astype(jnp.bfloat16)
    part_proj = jnp.dot(values.T, grad_proj, preferred_element_type=jnp.float32)
    grad_values = jnp.dot(grad_proj, proj_weight.T, preferred_element_type=jnp.float32).astype(jnp.bfloat16)
    part_value = jnp.dot(modulated.T, grad_values, preferred_element_type=jnp.float32)
    grad_mod = jnp.dot(grad_values, value_weight.T, preferred_element_type=jnp.float32)
    part_table = jnp.stack([lax.optimization_barrier(jnp.sum(grad_mod, axis=0)), lax.optimization_barrier(jnp.sum(grad_mod * normed, axis=0)), lax.optimization_barrier(jnp.sum(grad_up * projected, axis=0))])
    grad_norm = grad_mod * (1.0 + scale)
    centre_grad = lax.optimization_barrier(jnp.mean(grad_norm, axis=-1, keepdims=True))
    cross = lax.optimization_barrier(jnp.mean(grad_norm * normed, axis=-1, keepdims=True))
    grad_in = grad_up + inverse * (grad_norm - centre_grad - normed * cross)
    return (grad_in.astype(jnp.bfloat16), part_value, part_proj, part_table)

def reference(inputs, out_grad, guide_bin, time_step, guide_table, section_table, value_weight, proj_weight):
    condition = conditions(guide_bin, time_step, guide_table)
    rows_per = TOKENS // SAMPLES
    saved = []
    shared_all = []
    for batch in range(MICRO):
        shared = jnp.repeat(condition[batch], rows_per, axis=0)
        shared_all.append(shared)
        block_in = inputs[batch]
        kept = []
        for block in range(BLOCKS):
            modulation = shared + section_table[block].reshape(-1)
            kept.append(block_in)
            block_in = forward_block(block_in, modulation, value_weight[block], proj_weight[block])[0]
        saved.append(kept)
    value_sums = [jnp.zeros((D, H), jnp.float32) for index in range(BLOCKS)]
    proj_sums = [jnp.zeros((H, D), jnp.float32) for index in range(BLOCKS)]
    table_sums = [jnp.zeros((3, D), jnp.float32) for index in range(BLOCKS)]
    for batch in range(MICRO):
        upstream = out_grad[batch]
        for block in range(BLOCKS - 1, -1, -1):
            modulation = shared_all[batch] + section_table[block].reshape(-1)
            block_in = saved[batch][block]
            block_out, modulated, values, projected = forward_block(block_in, modulation, value_weight[block], proj_weight[block])
            upstream, part_value, part_proj, part_table = backward_block(block_in, modulated, values, projected, upstream, modulation, value_weight[block], proj_weight[block])
            value_sums[block] = value_sums[block] + part_value
            proj_sums[block] = proj_sums[block] + part_proj
            table_sums[block] = table_sums[block] + part_table
    return (jnp.stack(value_sums), jnp.stack(proj_sums), jnp.stack(table_sums))
```

```python
import functools
import math

import jax
import jax.numpy as jnp
from jax import lax
from jax.experimental import pallas as pl
from jax.experimental.pallas import tpu as pltpu
from jax.sharding import Mesh
from jax.sharding import PartitionSpec as P

DP = ("dp_0", "dp_1", "dp_2")

NORM_FLOOR = 0.1
PARTS = 2
CHUNK = 512


def conditions(guide_bin, time_step, guide_table):
    total = guide_table.shape[1]
    half = total // 2
    frequency = jnp.exp(-math.log(10000.0) * jnp.arange(half, dtype=jnp.float32) / half)
    angle = time_step.astype(jnp.float32)[..., None] * frequency
    waves = jnp.concatenate([jnp.sin(angle), jnp.cos(angle)], axis=-1)
    bin_count = guide_table.shape[0]
    onehot = (guide_bin[..., None] == jnp.arange(bin_count, dtype=jnp.int32)).astype(jnp.float32)
    picked = jnp.einsum(
        "msb,bw->msw", onehot, guide_table.astype(jnp.float32), precision=lax.Precision.HIGHEST
    )
    return picked + 0.5 * waves


def contract_rows(left, right):
    return lax.dot_general(
        left, right, (((0,), (0,)), ((), ())), preferred_element_type=jnp.float32
    )


def row_mean(value):
    return jnp.sum(value, axis=-1, keepdims=True) * (1.0 / value.shape[-1])


def normalize(hidden):
    centre = row_mean(hidden)
    centred = hidden - centre
    inverse = lax.rsqrt(row_mean(centred * centred) + NORM_FLOOR)
    return (centred * inverse, inverse)


def chosen_input(place, edge, direct, far, first_at, far_at):
    edge_value = edge[0]
    value = edge_value if direct is None else jnp.where(place == first_at, edge_value, direct[...])
    return value if far is None else jnp.where(place == far_at, far[...], value)


def forward_kernel(tick, units, has_direct, has_far, far_at, *refs):
    info, edge = refs[0], refs[1]
    rest = list(refs[2:])
    direct = rest.pop(0) if has_direct else None
    far = rest.pop(0) if has_far else None
    mod, value_weight, proj_weight = rest[:3]
    block_out, keep_in, keep_mod, keep_val, keep_proj = rest[-5:]
    unit = tick - info[1]

    @pl.when((unit >= 0) & (unit < units))
    def _():
        block_in = chosen_input(info[0], edge, direct, far, 0, far_at)
        keep_in[0] = block_in
        normed, _ = normalize(block_in.astype(jnp.float32))
        shift, scale = mod[0, 0:1, :], mod[0, 1:2, :]
        keep_mod[0] = (normed * (1.0 + scale) + shift).astype(jnp.bfloat16)

        def first(step, carry):
            at = pl.ds(pl.multiple_of(step * CHUNK, CHUNK), CHUNK)
            keep_val[0, :, at] = jnp.dot(
                keep_mod[0], value_weight[:, at], preferred_element_type=jnp.float32
            ).astype(jnp.bfloat16)
            return carry

        lax.fori_loop(0, value_weight.shape[1] // CHUNK, first, 0)

        def second(step, carry):
            at = pl.ds(pl.multiple_of(step * CHUNK, CHUNK), CHUNK)
            projected = jnp.dot(
                keep_val[0], proj_weight[:, at], preferred_element_type=jnp.float32
            )
            keep_proj[0, :, at] = projected
            hidden = keep_in[0, :, at].astype(jnp.float32)
            block_out[:, at] = (hidden + mod[0, 2:3, at] * projected).astype(jnp.bfloat16)
            return carry

        lax.fori_loop(0, proj_weight.shape[1] // CHUNK, second, 0)


def backward_kernel(tick, units, has_direct, has_far, first_at, far_at, *refs):
    info, edge = refs[0], refs[1]
    rest = list(refs[2:])
    direct = rest.pop(0) if has_direct else None
    far = rest.pop(0) if has_far else None
    mod, value_weight, proj_weight, keep_in, keep_proj, table_in = rest[:6]
    grad_in, keep_gval, keep_gproj, table_out, grad_mod = rest[-5:]
    unit = tick - info[2]
    valid = (unit >= 0) & (unit < units)

    @pl.when(jnp.logical_not(valid))
    def _():
        table_out[...] = table_in[...]

    @pl.when(valid)
    def _():
        upstream = chosen_input(info[0], edge, direct, far, first_at, far_at)
        grad_up = upstream.astype(jnp.float32)
        keep_gproj[0] = (mod[0, 2:3, :] * grad_up).astype(jnp.bfloat16)
        transposed = (((1,), (1,)), ((), ()))

        def first(step, carry):
            at = pl.ds(pl.multiple_of(step * CHUNK, CHUNK), CHUNK)
            keep_gval[0, :, at] = lax.dot_general(
                keep_gproj[0], proj_weight[at, :], transposed, preferred_element_type=jnp.float32
            ).astype(jnp.bfloat16)
            return carry

        lax.fori_loop(0, proj_weight.shape[0] // CHUNK, first, 0)

        def second(step, carry):
            at = pl.ds(pl.multiple_of(step * CHUNK, CHUNK), CHUNK)
            grad_mod[:, at] = lax.dot_general(
                keep_gval[0], value_weight[at, :], transposed, preferred_element_type=jnp.float32
            )
            return carry

        lax.fori_loop(0, value_weight.shape[0] // CHUNK, second, 0)
        normed, inverse = normalize(keep_in[0].astype(jnp.float32))
        grad = grad_mod[...]
        table_out[0:1, :] = table_in[0:1, :] + jnp.sum(grad, axis=0, keepdims=True)
        table_out[1:2, :] = table_in[1:2, :] + jnp.sum(grad * normed, axis=0, keepdims=True)
        table_out[2:3, :] = table_in[2:3, :] + jnp.sum(
            grad_up * keep_proj[0], axis=0, keepdims=True
        )
        grad_norm = grad * (1.0 + mod[0, 1:2, :])
        centre_grad = row_mean(grad_norm)
        cross = row_mean(grad_norm * normed)
        grad_in[...] = (grad_up + inverse * (grad_norm - centre_grad - normed * cross)).astype(
            jnp.bfloat16
        )


def swapped_sum(parts, axis):
    mine = lax.axis_index(axis)
    leaving = lax.dynamic_index_in_dim(parts, 1 - mine, 1, keepdims=False)
    staying = lax.dynamic_index_in_dim(parts, mine, 1, keepdims=False)
    arrived = lax.ppermute(leaving, axis, [(0, 1), (1, 0)])
    return staying.astype(jnp.float32) + arrived.astype(jnp.float32)


def sent_around(parts, axis):
    peers = lax.axis_size(axis)
    mine = lax.axis_index(axis)
    arrived = []
    for step in range(1, peers):
        leaving = lax.dynamic_index_in_dim(parts, (mine + step) % peers, 0, keepdims=False)
        pairs = [(source, (source + step) % peers) for source in range(peers)]
        arrived.append(lax.ppermute(leaving, axis, pairs))
    return [lax.dynamic_index_in_dim(parts, mine, 0, keepdims=False), *arrived]


def summed(parts):
    total = parts[0].astype(jnp.float32)
    for part in parts[1:]:
        total = total + part.astype(jnp.float32)
    return total


def scattered_sums(fulls):
    outer, inner, cores = (lax.axis_size(axis) for axis in DP)
    out = []
    ahead = None
    for full in fulls:
        rows, width = full.shape[0] // (outer * inner * cores), full.shape[1]
        parts = full.astype(jnp.bfloat16).reshape(outer * inner, cores, rows, width)
        parts = swapped_sum(parts, DP[2]).astype(jnp.bfloat16)
        parts = sent_around(parts.reshape(outer, inner * rows, width), DP[0])
        if ahead is not None:
            parts, ahead = lax.optimization_barrier((parts, ahead))
        ahead = summed(parts).astype(jnp.bfloat16)
        out.append(ahead.reshape(inner, rows, width))
    return [summed(sent_around(part, DP[1])) for part in out]


def summed_on_arrival(value, axis, dim):
    peers = lax.axis_size(axis)
    dims = value.shape
    parts = value.reshape(*dims[:dim], peers, dims[dim] // peers, *dims[dim + 1 :])
    parts = jnp.moveaxis(parts, dim, 0)
    arrived = lax.all_to_all(parts, axis, split_axis=0, concat_axis=0, tiled=True)
    return arrived.sum(axis=0)


def per_device(
    inputs, out_grad, guide_bin, time_step, guide_table, section_table, value_weight, proj_weight
):
    sections = lax.axis_size("section")
    place = lax.axis_index("section")
    batches, tok_dev, width = inputs.shape
    value_width = value_weight.shape[2]
    rows = tok_dev // PARTS
    units = batches * PARTS
    slots = units + 1
    far = sections // 2
    delay = [s + (s >= far) for s in range(sections)]
    back_delay = [delay[sections - 1 - s] for s in range(sections)]
    depth = delay[-1]

    condition = conditions(guide_bin, time_step, guide_table)[:, 0]
    modulation = (condition + section_table[0].reshape(-1)).reshape(batches, 3, width)
    value_weight = value_weight[0]
    proj_weight = proj_weight[0]
    edge_in = inputs.reshape(units, rows, width)
    edge_grad = out_grad.reshape(units, rows, width)
    late = (place >= far).astype(jnp.int32)
    info = jnp.stack([place, place + late, sections - 1 - place + 1 - late]).astype(jnp.int32)

    block = (1, rows, width)
    act = lambda: pl.BlockSpec((rows, width), lambda i, s: (0, 0))
    whole = lambda shape: pl.BlockSpec(shape, lambda i, s: (0,) * len(shape))
    anywhere = pl.BlockSpec(memory_space=pl.ANY)
    resident = pl.BlockSpec(memory_space=pltpu.VMEM)
    value_weight = pltpu.with_memory_space_constraint(value_weight, pltpu.VMEM)
    proj_weight = pltpu.with_memory_space_constraint(proj_weight, pltpu.VMEM)

    def read_slot(tick, which):
        return lambda i, s: (jnp.clip(tick - s[which], 0, units - 1), 0, 0)

    def write_slot(tick, which):
        def index(i, s):
            unit = tick - s[which]
            return (jnp.where((unit >= 0) & (unit < units), unit, units), 0, 0)

        return index

    def mod_spec(tick, which):
        return pl.BlockSpec(
            (1, 3, width),
            lambda i, s: (lax.div(jnp.clip(tick - s[which], 0, units - 1), PARTS), 0, 0),
        )

    flops = 4 * rows * width * value_width
    cost = pl.CostEstimate(flops=flops, bytes_accessed=16 * rows * width, transcendentals=0)
    params = pltpu.CompilerParams(
        dimension_semantics=("arbitrary",), vmem_limit_bytes=10 * 1024 * 1024
    )

    def forward(tick, direct, distant, kept):
        extra = [value for value in (direct, distant) if value is not None]
        lead = 1 + 1 + len(extra) + 3
        spec = pltpu.PrefetchScalarGridSpec(
            num_scalar_prefetch=1,
            grid=(1,),
            in_specs=[pl.BlockSpec(block, read_slot(tick, 1))]
            + [act() for _ in extra]
            + [mod_spec(tick, 1), resident, resident]
            + [anywhere] * 4,
            out_specs=[act()] + [pl.BlockSpec(block, write_slot(tick, 1)) for _ in range(4)],
        )
        return pl.pallas_call(
            functools.partial(
                forward_kernel, tick, units, direct is not None, distant is not None, far
            ),
            grid_spec=spec,
            out_shape=[jax.ShapeDtypeStruct((rows, width), jnp.bfloat16)]
            + [jax.ShapeDtypeStruct(k.shape, k.dtype) for k in kept],
            input_output_aliases={lead + i: 1 + i for i in range(4)},
            cost_estimate=cost,
            compiler_params=params,
            name="fwd",
        )(info, edge_in, *extra, modulation, value_weight, proj_weight, *kept)

    def backward(tick, direct, distant, keep_in, keep_proj, stores, table):
        extra = [value for value in (direct, distant) if value is not None]
        lead = 1 + 1 + len(extra) + 3 + 2
        spec = pltpu.PrefetchScalarGridSpec(
            num_scalar_prefetch=1,
            grid=(1,),
            in_specs=[pl.BlockSpec(block, read_slot(tick, 2))]
            + [act() for _ in extra]
            + [mod_spec(tick, 2), resident, resident]
            + [pl.BlockSpec(block, read_slot(tick, 2)) for _ in range(2)]
            + [whole((3, width)), anywhere, anywhere],
            out_specs=[act()]
            + [pl.BlockSpec(block, write_slot(tick, 2)) for _ in range(2)]
            + [whole((3, width))],
            scratch_shapes=[pltpu.VMEM((rows, width), jnp.float32)],
        )
        return pl.pallas_call(
            functools.partial(
                backward_kernel,
                tick,
                units,
                direct is not None,
                distant is not None,
                sections - 1,
                far - 1,
            ),
            grid_spec=spec,
            out_shape=[jax.ShapeDtypeStruct((rows, width), jnp.bfloat16)]
            + [jax.ShapeDtypeStruct(k.shape, k.dtype) for k in stores]
            + [jax.ShapeDtypeStruct((3, width), jnp.float32)],
            input_output_aliases={lead: 3, lead + 1: 1, lead + 2: 2},
            cost_estimate=cost,
            compiler_params=params,
            name="bwd",
        )(
            info,
            edge_grad,
            *extra,
            modulation,
            value_weight,
            proj_weight,
            keep_in,
            keep_proj,
            table,
            *stores,
        )

    def send(value, tick, delays, step, is_far):
        pairs = []
        for s in range(sections):
            to = s + step
            if not 0 <= to < sections or not 0 <= tick - delays[s] < units:
                continue
            if ((s < far) != (to < far)) == is_far:
                pairs.append((s, to))
        return lax.ppermute(value, "section", pairs) if pairs else None

    def kept_like(dtype):
        return jnp.zeros((slots, rows, width), dtype)

    kept = [kept_like(jnp.bfloat16) for _ in range(3)] + [kept_like(jnp.float32)]
    stores = [kept_like(jnp.bfloat16) for _ in range(2)]
    table = jnp.zeros((3, width), jnp.float32)
    near_f, far_f, near_b, far_b = {}, {}, {}, {}
    for tick in range(2 * depth + units):
        if tick < depth + units:
            block_out, *kept = forward(tick, near_f.get(tick), far_f.get(tick), kept)
            near_f[tick + 1] = send(block_out, tick, delay, 1, False)
            far_f[tick + 2] = send(block_out, tick, delay, 1, True)
        back = tick - depth
        if back >= 0:
            grad_in, *rest = backward(
                back, near_b.get(back), far_b.get(back), kept[0], kept[3], stores, table
            )
            stores, table = rest[:2], rest[2]
            near_b[back + 1] = send(grad_in, back, back_delay, -1, False)
            far_b[back + 2] = send(grad_in, back, back_delay, -1, True)

    def flat(value):
        return value[:units].reshape(units * rows, -1)

    value_full = contract_rows(flat(kept[1]), flat(stores[0]))
    proj_full = contract_rows(flat(kept[2]), flat(stores[1]))
    value_part, proj_part = scattered_sums((value_full, proj_full))
    table_part = summed_on_arrival(table, DP, 1)
    return (value_part[None], proj_part[None], table_part[None])


def solution(mesh):
    finer = Mesh(
        mesh.devices.reshape(mesh.shape["section"], 4, 4, 2), ("section", "dp_0", "dp_1", "dp_2")
    )
    placed = (
        P(None, DP, None),
        P(None, DP, None),
        P(),
        P(),
        P(),
        P("section", None, None),
        P("section", None, None),
        P("section", None, None),
    )
    return jax.shard_map(
        per_device,
        mesh=finer,
        in_specs=placed,
        out_specs=(P("section", DP, None), P("section", DP, None), P("section", None, DP)),
        check_vma=False,
    )
```

```python
import functools
import math

import jax
import jax.numpy as jnp
from jax import lax
from jax.experimental import pallas as pl
from jax.experimental.pallas import tpu as pltpu
from jax.sharding import Mesh
from jax.sharding import PartitionSpec as P

DP = ("dp_0", "dp_1", "dp_2")

NORM_FLOOR = 0.1
PARTS = 2
CHUNK = 512
PCHUNK = 512
BLOCK = 384
GROUP = 16


def conditions(guide_bin, time_step, guide_table):
    total = guide_table.shape[1]
    half = total // 2
    frequency = jnp.exp(-math.log(10000.0) * jnp.arange(half, dtype=jnp.float32) / half)
    angle = time_step.astype(jnp.float32)[..., None] * frequency
    waves = jnp.concatenate([jnp.sin(angle), jnp.cos(angle)], axis=-1)
    bin_count = guide_table.shape[0]
    onehot = (guide_bin[..., None] == jnp.arange(bin_count, dtype=jnp.int32)).astype(jnp.float32)
    picked = jnp.einsum(
        "msb,bw->msw", onehot, guide_table.astype(jnp.float32), precision=lax.Precision.HIGHEST
    )
    return picked + 0.5 * waves


def row_mean(value):
    return jnp.sum(value, axis=-1, keepdims=True) * (1.0 / value.shape[-1])


def normalize(hidden):
    centre = row_mean(hidden)
    centred = hidden - centre
    inverse = lax.rsqrt(row_mean(centred * centred) + NORM_FLOOR)
    return (centred * inverse, inverse)


def chosen_input(place, unit, at, edge, direct, far, first_at, far_at):
    value = edge[unit, at, :]
    if direct is not None:
        value = jnp.where(place == first_at, value, direct[at, :])
    return value if far is None else jnp.where(place == far_at, far[at, :], value)


def row_groups(rows, body):
    def step(index, carry):
        body(pl.ds(pl.multiple_of(index * GROUP, GROUP), GROUP))
        return carry

    lax.fori_loop(0, rows // GROUP, step, 0)


def column_chunks(columns, body):
    def step(index, carry):
        body(pl.ds(pl.multiple_of(index * CHUNK, CHUNK), CHUNK))
        return carry

    lax.fori_loop(0, columns // CHUNK, step, 0)


def forward_kernel(tick, units, has_direct, has_far, far_at, *refs):
    info, edge = refs[0], refs[1]
    rest = list(refs[2:])
    direct = rest.pop(0) if has_direct else None
    far = rest.pop(0) if has_far else None
    mod, value_weight, proj_weight = rest[:3]
    block_out, keep_in, keep_mod, keep_val, keep_proj = rest[-5:]
    unit = tick - info[1]
    batch = lax.div(unit, PARTS)

    @pl.when((unit >= 0) & (unit < units))
    def _():
        def modulate(at):
            block_in = chosen_input(info[0], unit, at, edge, direct, far, 0, far_at)
            keep_in[unit, at, :] = block_in
            normed, _ = normalize(block_in.astype(jnp.float32))
            shift, scale = mod[batch, 0:1, :], mod[batch, 1:2, :]
            keep_mod[unit, at, :] = (normed * (1.0 + scale) + shift).astype(jnp.bfloat16)

        row_groups(block_out.shape[0], modulate)

        def first(at):
            keep_val[unit, :, at] = jnp.dot(
                keep_mod[unit], value_weight[:, at], preferred_element_type=jnp.float32
            ).astype(jnp.bfloat16)

        column_chunks(value_weight.shape[1], first)

        def second(at):
            projected = jnp.dot(
                keep_val[unit], proj_weight[:, at], preferred_element_type=jnp.float32
            )
            keep_proj[unit, :, at] = projected
            hidden = keep_in[unit, :, at].astype(jnp.float32)
            block_out[:, at] = (hidden + mod[batch, 2:3, at] * projected).astype(jnp.bfloat16)

        column_chunks(proj_weight.shape[1], second)


def backward_kernel(tick, units, has_direct, has_far, first_at, far_at, has_table, *refs):
    info, edge = refs[0], refs[1]
    rest = list(refs[2:])
    direct = rest.pop(0) if has_direct else None
    far = rest.pop(0) if has_far else None
    mod, value_weight, proj_weight, keep_in, keep_proj = rest[:5]
    table_in = rest[5] if has_table else None
    grad_in, keep_gval, keep_gproj, table_out, grad_mod, sums = rest[-6:]
    unit = tick - info[2]
    batch = lax.div(unit, PARTS)
    valid = (unit >= 0) & (unit < units)
    rows, width = grad_in.shape

    @pl.when(jnp.logical_not(valid))
    def _():
        table_out[...] = jnp.zeros_like(table_out) if table_in is None else table_in[...]

    @pl.when(valid)
    def _():
        def upstream(at):
            return chosen_input(info[0], unit, at, edge, direct, far, first_at, far_at).astype(
                jnp.float32
            )

        def gated(at):
            keep_gproj[unit, at, :] = (mod[batch, 2:3, :] * upstream(at)).astype(jnp.bfloat16)

        row_groups(rows, gated)
        transposed = (((1,), (1,)), ((), ()))

        def first(at):
            keep_gval[unit, :, at] = lax.dot_general(
                keep_gproj[unit], proj_weight[at, :], transposed, preferred_element_type=jnp.float32
            ).astype(jnp.bfloat16)

        column_chunks(proj_weight.shape[0], first)

        def second(at):
            grad_mod[:, at] = lax.dot_general(
                keep_gval[unit], value_weight[at, :], transposed, preferred_element_type=jnp.float32
            )

        column_chunks(value_weight.shape[0], second)
        sums[...] = jnp.zeros_like(sums)

        def finish(at):
            normed, inverse = normalize(keep_in[unit, at, :].astype(jnp.float32))
            grad, grad_up = grad_mod[at, :], upstream(at)
            for index, term in enumerate((grad, grad * normed, grad_up * keep_proj[unit, at, :])):
                sums[index] += jnp.sum(term.reshape(GROUP // 8, 8, width), axis=0)
            grad_norm = grad * (1.0 + mod[batch, 1:2, :])
            centre_grad = row_mean(grad_norm)
            cross = row_mean(grad_norm * normed)
            grad_in[at, :] = (
                grad_up + inverse * (grad_norm - centre_grad - normed * cross)
            ).astype(jnp.bfloat16)

        row_groups(rows, finish)
        for index in range(3):
            total = jnp.sum(sums[index], axis=0, keepdims=True)
            table_out[index : index + 1, :] = (
                total if table_in is None else table_in[index : index + 1, :] + total
            )


def product_kernel(core, left, right, leaving, staying, tall):
    depth = left.shape[0] * left.shape[1]
    rows = leaving.shape[1]
    tall[...] = jnp.transpose(left[...].reshape(depth, left.shape[2]))
    pairs = BLOCK // (2 * rows)
    chunks = right.shape[2] // PCHUNK

    def block(step, carry):
        down = lax.div(step, chunks)
        at = pl.ds(pl.multiple_of(lax.rem(step, chunks) * PCHUNK, PCHUNK), PCHUNK)
        total = jnp.dot(
            tall[pl.ds(pl.multiple_of(down * BLOCK, BLOCK), BLOCK), :],
            right[:, :, at].reshape(depth, PCHUNK),
            preferred_element_type=jnp.float32,
        ).astype(jnp.bfloat16)
        for pair in range(pairs):
            even = total[(2 * pair) * rows : (2 * pair + 1) * rows]
            odd = total[(2 * pair + 1) * rows : (2 * pair + 2) * rows]
            group = down * pairs + pair
            staying[group, :, at] = jnp.where(core[0] == 0, even, odd)
            leaving[group, :, at] = jnp.where(core[0] == 0, odd, even)
        return carry

    lax.fori_loop(0, tall.shape[0] // BLOCK * chunks, block, 0)


def swapped_product(left, right, core):
    outer, inner, cores = (lax.axis_size(axis) for axis in DP)
    units, unit_rows, width = right.shape
    rows = left.shape[2] // (outer * inner * cores)
    whole = jax.ShapeDtypeStruct((outer * inner, rows, width), jnp.bfloat16)
    vmem = pl.BlockSpec(memory_space=pltpu.VMEM)
    leaving, staying = pl.pallas_call(
        product_kernel,
        in_specs=[pl.BlockSpec(memory_space=pltpu.SMEM), vmem, vmem],
        out_specs=[vmem, vmem],
        out_shape=[whole, whole],
        scratch_shapes=[pltpu.VMEM((left.shape[2], units * unit_rows), jnp.bfloat16)],
        cost_estimate=pl.CostEstimate(
            flops=2 * units * unit_rows * left.shape[2] * width,
            bytes_accessed=2 * left.shape[2] * width,
            transcendentals=0,
        ),
        compiler_params=pltpu.CompilerParams(vmem_limit_bytes=12 * 1024 * 1024),
        name="product",
    )(core, left, right)
    arrived = lax.ppermute(leaving, DP[2], [(0, 1), (1, 0)])
    return staying.astype(jnp.float32) + arrived.astype(jnp.float32)


def sent_around(parts, axis, turns):
    peers = lax.axis_size(axis)
    arrived = []
    for step in range(1, peers):
        leaving = lax.dynamic_index_in_dim(parts, turns[step], 0, keepdims=False)
        pairs = [(source, (source + step) % peers) for source in range(peers)]
        arrived.append(lax.ppermute(leaving, axis, pairs))
    return [lax.dynamic_index_in_dim(parts, turns[0], 0, keepdims=False), *arrived]


def summed(parts):
    total = parts[0].astype(jnp.float32)
    for part in parts[1:]:
        total = total + part.astype(jnp.float32)
    return total


def scattered_products(pairs, core, outer_turns, inner_turns):
    outer, inner = (lax.axis_size(axis) for axis in DP[:2])
    out = []
    for left, right in pairs:
        parts = swapped_product(left, right, core).astype(jnp.bfloat16)
        rows, width = parts.shape[1:]
        parts = sent_around(parts.reshape(outer, inner * rows, width), DP[0], outer_turns)
        if out:
            parts, out[-1] = lax.optimization_barrier((parts, out[-1]))
        parts = summed(parts).astype(jnp.bfloat16).reshape(inner, rows, width)
        out.append(sent_around(parts, DP[1], inner_turns))
    return [summed(parts) for parts in out]


def summed_on_arrival(value, axis, dim):
    peers = lax.axis_size(axis)
    dims = value.shape
    parts = value.reshape(*dims[:dim], peers, dims[dim] // peers, *dims[dim + 1 :])
    parts = jnp.moveaxis(parts, dim, 0)
    arrived = lax.all_to_all(parts, axis, split_axis=0, concat_axis=0, tiled=True)
    return arrived.sum(axis=0)


def per_device(
    inputs, out_grad, guide_bin, time_step, guide_table, section_table, value_weight, proj_weight
):
    sections = lax.axis_size("section")
    place = lax.axis_index("section")
    batches, tok_dev, width = inputs.shape
    value_width = value_weight.shape[2]
    rows = tok_dev // PARTS
    units = batches * PARTS
    far = sections // 2
    delay = [s + (s >= far) for s in range(sections)]
    back_delay = [delay[sections - 1 - s] for s in range(sections)]
    depth = delay[-1]

    condition = conditions(guide_bin, time_step, guide_table)[:, 0]
    modulation = (condition + section_table[0].reshape(-1)).reshape(batches, 3, width)
    value_weight = value_weight[0]
    proj_weight = proj_weight[0]
    edge_in = inputs.reshape(units, rows, width)
    edge_grad = out_grad.reshape(units, rows, width)
    late = (place >= far).astype(jnp.int32)
    info = jnp.stack([place, place + late, sections - 1 - place + 1 - late]).astype(jnp.int32)
    core = lax.axis_index(DP[2]).astype(jnp.int32).reshape(1)
    turns = [
        [(lax.axis_index(axis) + step) % lax.axis_size(axis) for step in range(lax.axis_size(axis))]
        for axis in DP[:2]
    ]
    info, core, (outer_turns, inner_turns) = lax.optimization_barrier((info, core, turns))

    vmem = pl.BlockSpec(memory_space=pltpu.VMEM)
    smem = pl.BlockSpec(memory_space=pltpu.SMEM)
    value_weight, proj_weight, edge_in, edge_grad = (
        pltpu.with_memory_space_constraint(value, pltpu.VMEM)
        for value in (value_weight, proj_weight, edge_in, edge_grad)
    )

    def slots_of(dtype):
        return jax.ShapeDtypeStruct((units, rows, width), dtype)

    flops = 4 * rows * width * value_width
    cost = pl.CostEstimate(flops=flops, bytes_accessed=16 * rows * width, transcendentals=0)
    params = pltpu.CompilerParams(vmem_limit_bytes=10 * 1024 * 1024)
    hop = jax.ShapeDtypeStruct((rows, width), jnp.bfloat16)

    def forward(tick, direct, distant, kept):
        extra = [value for value in (direct, distant) if value is not None]
        operands = (info, edge_in, *extra, modulation, value_weight, proj_weight, *kept)
        lead = len(operands) - len(kept)
        return pl.pallas_call(
            functools.partial(
                forward_kernel, tick, units, direct is not None, distant is not None, far
            ),
            in_specs=[smem] + [vmem] * (len(operands) - 1),
            out_specs=[vmem] * 5,
            out_shape=[hop]
            + [slots_of(dtype) for dtype in (jnp.bfloat16, jnp.bfloat16, jnp.bfloat16, jnp.float32)],
            input_output_aliases={lead + i: 1 + i for i in range(len(kept))},
            cost_estimate=cost,
            compiler_params=params,
            name="fwd",
        )(*operands)

    def backward(tick, direct, distant, keep_in, keep_proj, sofar):
        extra = [value for value in (direct, distant) if value is not None]
        operands = (
            info,
            edge_grad,
            *extra,
            modulation,
            value_weight,
            proj_weight,
            keep_in,
            keep_proj,
            *sofar,
        )
        lead = len(operands) - len(sofar)
        return pl.pallas_call(
            functools.partial(
                backward_kernel,
                tick,
                units,
                direct is not None,
                distant is not None,
                sections - 1,
                far - 1,
                bool(sofar),
            ),
            in_specs=[smem] + [vmem] * (len(operands) - 1),
            out_specs=[vmem] * 4,
            out_shape=[hop]
            + [slots_of(jnp.bfloat16)] * 2
            + [jax.ShapeDtypeStruct((3, width), jnp.float32)],
            input_output_aliases={lead: 3, lead + 1: 1, lead + 2: 2} if sofar else {},
            scratch_shapes=[
                pltpu.VMEM((rows, width), jnp.float32),
                pltpu.VMEM((3, 8, width), jnp.float32),
            ],
            cost_estimate=cost,
            compiler_params=params,
            name="bwd",
        )(*operands)

    def send(value, tick, delays, step, is_far):
        pairs, wanted = [], False
        for s in range(sections):
            to = s + step
            if 0 <= to < sections and ((s < far) != (to < far)) == is_far:
                pairs.append((s, to))
                wanted = wanted or 0 <= tick - delays[s] < units
        return lax.ppermute(value, "section", pairs) if wanted else None

    kept, sofar = [], []
    near_f, far_f, near_b, far_b = {}, {}, {}, {}
    for tick in range(2 * depth + units):
        if tick < depth + units:
            block_out, *kept = forward(tick, near_f.get(tick), far_f.get(tick), kept)
            near_f[tick + 1] = send(block_out, tick, delay, 1, False)
            far_f[tick + 2] = send(block_out, tick, delay, 1, True)
        back = tick - depth
        if back >= 0:
            grad_in, *rest = backward(
                back, near_b.get(back), far_b.get(back), kept[0], kept[3], sofar
            )
            sofar = [rest[2], rest[0], rest[1]]
            near_b[back + 1] = send(grad_in, back, back_delay, -1, False)
            far_b[back + 2] = send(grad_in, back, back_delay, -1, True)

    value_part, proj_part = scattered_products(
        ((kept[1], sofar[1]), (kept[2], sofar[2])), core, outer_turns, inner_turns
    )
    table_part = summed_on_arrival(sofar[0], DP, 1)
    return (value_part[None], proj_part[None], table_part[None])


def solution(mesh):
    finer = Mesh(
        mesh.devices.reshape(mesh.shape["section"], 4, 4, 2), ("section", "dp_0", "dp_1", "dp_2")
    )
    placed = (
        P(None, DP, None),
        P(None, DP, None),
        P(),
        P(),
        P(),
        P("section", None, None),
        P("section", None, None),
        P("section", None, None),
    )
    return jax.shard_map(
        per_device,
        mesh=finer,
        in_specs=placed,
        out_specs=(P("section", DP, None), P("section", DP, None), P("section", None, DP)),
        check_vma=False,
    )
```

```python
import functools
import math

import jax
import jax.numpy as jnp
from jax import lax
from jax.experimental import pallas as pl
from jax.experimental.pallas import tpu as pltpu
from jax.sharding import Mesh
from jax.sharding import PartitionSpec as P

DP = ("dp_0", "dp_1", "dp_2")

NORM_FLOOR = 0.1
PARTS = 2
CHUNK = 512
PCHUNK = 512
BLOCK = 384
GROUP = 64


def conditions(guide_bin, time_step, guide_table):
    total = guide_table.shape[1]
    half = total // 2
    frequency = jnp.exp(-math.log(10000.0) * jnp.arange(half, dtype=jnp.float32) / half)
    angle = time_step.astype(jnp.float32)[..., None] * frequency
    waves = jnp.concatenate([jnp.sin(angle), jnp.cos(angle)], axis=-1)
    bin_count = guide_table.shape[0]
    onehot = (guide_bin[..., None] == jnp.arange(bin_count, dtype=jnp.int32)).astype(jnp.float32)
    picked = jnp.einsum(
        "msb,bw->msw", onehot, guide_table.astype(jnp.float32), precision=lax.Precision.HIGHEST
    )
    return picked + 0.5 * waves


def row_mean(value):
    return jnp.sum(value, axis=-1, keepdims=True) * (1.0 / value.shape[-1])


def normalize(hidden):
    centre = row_mean(hidden)
    centred = hidden - centre
    inverse = lax.rsqrt(row_mean(centred * centred) + NORM_FLOOR)
    return (centred * inverse, inverse)


def chosen_input(place, unit, at, edge, direct, far, first_at, far_at):
    value = edge[unit, at, :]
    if direct is not None:
        value = jnp.where(place == first_at, value, direct[at, :])
    return value if far is None else jnp.where(place == far_at, far[at, :], value)


def row_groups(rows, body):
    def step(index, carry):
        body(pl.ds(pl.multiple_of(index * GROUP, GROUP), GROUP))
        return carry

    lax.fori_loop(0, rows // GROUP, step, 0)


def column_chunks(columns, body):
    def step(index, carry):
        body(pl.ds(pl.multiple_of(index * CHUNK, CHUNK), CHUNK))
        return carry

    lax.fori_loop(0, columns // CHUNK, step, 0)


def forward_kernel(tick, units, has_direct, has_far, far_at, *refs):
    info, edge = refs[0], refs[1]
    rest = list(refs[2:])
    direct = rest.pop(0) if has_direct else None
    far = rest.pop(0) if has_far else None
    mod, value_weight, proj_weight = rest[:3]
    block_out, keep_in, keep_mod, keep_val, keep_proj = rest[-5:]
    unit = tick - info[1]
    batch = lax.div(unit, PARTS)

    @pl.when((unit >= 0) & (unit < units))
    def _():
        def modulate(at):
            block_in = chosen_input(info[0], unit, at, edge, direct, far, 0, far_at)
            keep_in[unit, at, :] = block_in
            normed, _ = normalize(block_in.astype(jnp.float32))
            shift, scale = mod[batch, 0:1, :], mod[batch, 1:2, :]
            keep_mod[unit, at, :] = (normed * (1.0 + scale) + shift).astype(jnp.bfloat16)

        row_groups(block_out.shape[0], modulate)

        def first(at):
            keep_val[unit, :, at] = jnp.dot(
                keep_mod[unit], value_weight[:, at], preferred_element_type=jnp.float32
            ).astype(jnp.bfloat16)

        column_chunks(value_weight.shape[1], first)

        def second(at):
            projected = jnp.dot(
                keep_val[unit], proj_weight[:, at], preferred_element_type=jnp.float32
            )
            keep_proj[unit, :, at] = projected
            hidden = keep_in[unit, :, at].astype(jnp.float32)
            block_out[:, at] = (hidden + mod[batch, 2:3, at] * projected).astype(jnp.bfloat16)

        column_chunks(proj_weight.shape[1], second)


def gate_kernel(tick, units, has_direct, has_far, first_at, far_at, *refs):
    info, edge = refs[0], refs[1]
    rest = list(refs[2:])
    direct = rest.pop(0) if has_direct else None
    far = rest.pop(0) if has_far else None
    mod, keep_gproj = rest[0], rest[-1]
    unit = tick - info[2]

    @pl.when((unit >= 0) & (unit < units))
    def _():
        def gated(at):
            upstream = chosen_input(info[0], unit, at, edge, direct, far, first_at, far_at)
            keep_gproj[unit, at, :] = (
                mod[lax.div(unit, PARTS), 2:3, :] * upstream.astype(jnp.float32)
            ).astype(jnp.bfloat16)

        row_groups(keep_gproj.shape[1], gated)


def backward_kernel(
    tick, units, has_direct, has_far, first_at, far_at, has_table, final, *refs
):
    info, edge = refs[0], refs[1]
    rest = list(refs[2:])
    direct = rest.pop(0) if has_direct else None
    far = rest.pop(0) if has_far else None
    mod, value_weight, proj_weight, keep_in, keep_proj = rest[:5]
    table_in = rest[5] if has_table else None
    grad_mod, sums = rest[-2:]
    if final:
        keep_gproj = rest[7]
        keep_gval, table_out = rest[-4:-2]
    else:
        grad_in, keep_gval, keep_gproj, table_out = rest[-6:-2]
    unit = tick - info[2]
    batch = lax.div(unit, PARTS)
    valid = (unit >= 0) & (unit < units)
    rows, width = grad_mod.shape

    @pl.when(jnp.logical_not(valid))
    def _():
        table_out[...] = jnp.zeros_like(table_out) if table_in is None else table_in[...]

    @pl.when(valid)
    def _():
        def upstream(at):
            return chosen_input(info[0], unit, at, edge, direct, far, first_at, far_at).astype(
                jnp.float32
            )

        def gated(at):
            keep_gproj[unit, at, :] = (mod[batch, 2:3, :] * upstream(at)).astype(jnp.bfloat16)

        if not final:
            row_groups(rows, gated)
        transposed = (((1,), (1,)), ((), ()))

        def first(at):
            keep_gval[unit, :, at] = lax.dot_general(
                keep_gproj[unit], proj_weight[at, :], transposed, preferred_element_type=jnp.float32
            ).astype(jnp.bfloat16)

        column_chunks(proj_weight.shape[0], first)

        def second(at):
            grad_mod[:, at] = lax.dot_general(
                keep_gval[unit], value_weight[at, :], transposed, preferred_element_type=jnp.float32
            )

        column_chunks(value_weight.shape[0], second)
        sums[...] = jnp.zeros_like(sums)

        def finish(at):
            normed, inverse = normalize(keep_in[unit, at, :].astype(jnp.float32))
            grad, grad_up = grad_mod[at, :], upstream(at)
            for index, term in enumerate((grad, grad * normed, grad_up * keep_proj[unit, at, :])):
                sums[index] += jnp.sum(term.reshape(GROUP // 8, 8, width), axis=0)
            if final:
                return
            grad_norm = grad * (1.0 + mod[batch, 1:2, :])
            centre_grad = row_mean(grad_norm)
            cross = row_mean(grad_norm * normed)
            grad_in[at, :] = (
                grad_up + inverse * (grad_norm - centre_grad - normed * cross)
            ).astype(jnp.bfloat16)

        row_groups(rows, finish)
        for index in range(3):
            total = jnp.sum(sums[index], axis=0, keepdims=True)
            table_out[index : index + 1, :] = (
                total if table_in is None else table_in[index : index + 1, :] + total
            )


def product_kernel(core, left, right, leaving, staying, tall):
    depth = left.shape[0] * left.shape[1]
    rows = leaving.shape[1]
    tall[...] = jnp.transpose(left[...].reshape(depth, left.shape[2]))
    pairs = BLOCK // (2 * rows)
    chunks = right.shape[2] // PCHUNK

    def block(step, carry):
        down = lax.div(step, chunks)
        at = pl.ds(pl.multiple_of(lax.rem(step, chunks) * PCHUNK, PCHUNK), PCHUNK)
        total = jnp.dot(
            tall[pl.ds(pl.multiple_of(down * BLOCK, BLOCK), BLOCK), :],
            right[:, :, at].reshape(depth, PCHUNK),
            preferred_element_type=jnp.float32,
        ).astype(jnp.bfloat16)
        for pair in range(pairs):
            even = total[(2 * pair) * rows : (2 * pair + 1) * rows]
            odd = total[(2 * pair + 1) * rows : (2 * pair + 2) * rows]
            group = down * pairs + pair
            staying[group, :, at] = jnp.where(core[0] == 0, even, odd)
            leaving[group, :, at] = jnp.where(core[0] == 0, odd, even)
        return carry

    lax.fori_loop(0, tall.shape[0] // BLOCK * chunks, block, 0)


def split_product(left, right, core):
    outer, inner, cores = (lax.axis_size(axis) for axis in DP)
    units, unit_rows, width = right.shape
    rows = left.shape[2] // (outer * inner * cores)
    whole = jax.ShapeDtypeStruct((outer * inner, rows, width), jnp.bfloat16)
    vmem = pl.BlockSpec(memory_space=pltpu.VMEM)
    return pl.pallas_call(
        product_kernel,
        in_specs=[pl.BlockSpec(memory_space=pltpu.SMEM), vmem, vmem],
        out_specs=[vmem, vmem],
        out_shape=[whole, whole],
        scratch_shapes=[pltpu.VMEM((left.shape[2], units * unit_rows), jnp.bfloat16)],
        cost_estimate=pl.CostEstimate(
            flops=2 * units * unit_rows * left.shape[2] * width,
            bytes_accessed=2 * left.shape[2] * width,
            transcendentals=0,
        ),
        compiler_params=pltpu.CompilerParams(vmem_limit_bytes=12 * 1024 * 1024),
        name="product",
    )(core, left, right)


def taken(parts, index):
    return lax.dynamic_index_in_dim(parts, index, 0, keepdims=False)


def summed(*parts):
    total = parts[0].astype(jnp.float32)
    for part in parts[1:]:
        total = total + part.astype(jnp.float32)
    return total


def turned(value, axis, step):
    peers = lax.axis_size(axis)
    return lax.ppermute(value, axis, [(i, (i + step) % peers) for i in range(peers)])


def swapped_sum(leaving, staying):
    arrived = lax.ppermute(leaving, DP[2], [(0, 1), (1, 0)])
    return summed(staying, arrived).astype(jnp.bfloat16)


def ring_parts(parts, turns):
    middle = parts.shape[1] // 2
    across = taken(parts, turns[2])
    above = turned(across[:middle], DP[0], 1)
    below = turned(across[middle:], DP[0], -1)
    ahead, behind = taken(parts, turns[1]), taken(parts, turns[3])
    ahead = jnp.concatenate(
        [summed(ahead[:middle], above).astype(jnp.bfloat16), ahead[middle:]], axis=0
    )
    behind = jnp.concatenate(
        [behind[:middle], summed(behind[middle:], below).astype(jnp.bfloat16)], axis=0
    )
    return [taken(parts, turns[0]), turned(ahead, DP[0], 1), turned(behind, DP[0], -1)]


def sent_around(parts, turns, leaving):
    arrived = [turned(part, DP[1], step) for step, part in enumerate(leaving, 1)]
    return [taken(parts, turns[0]), *arrived]


def scattered(halves, outer_turns, inner_turns, ahead, table):
    outer, inner = (lax.axis_size(axis) for axis in DP[:2])
    parts = swapped_sum(*halves)
    rows, width = parts.shape[1:]
    parts = ring_parts(parts.reshape(outer, inner * rows, width), outer_turns)
    if ahead is not None:
        parts, ahead = lax.optimization_barrier((parts, ahead))
    parts = summed(*parts).astype(jnp.bfloat16).reshape(inner, rows, width)
    leaving = [taken(parts, turn) for turn in inner_turns[1:]]
    if table is not None:
        leaving, table = lax.optimization_barrier((leaving, table))
    return sent_around(parts, inner_turns, leaving), ahead, table


def summed_on_arrival(value, axis, dim):
    peers = lax.axis_size(axis)
    dims = value.shape
    parts = value.reshape(*dims[:dim], peers, dims[dim] // peers, *dims[dim + 1 :])
    parts = jnp.moveaxis(parts, dim, 0)
    arrived = lax.all_to_all(parts, axis, split_axis=0, concat_axis=0, tiled=True)
    return arrived.sum(axis=0)


def per_device(
    inputs, out_grad, guide_bin, time_step, guide_table, section_table, value_weight, proj_weight
):
    sections = lax.axis_size("section")
    place = lax.axis_index("section")
    batches, tok_dev, width = inputs.shape
    value_width = value_weight.shape[2]
    rows = tok_dev // PARTS
    units = batches * PARTS
    far = sections // 2
    delay = [s + (s >= far) for s in range(sections)]
    back_delay = [delay[sections - 1 - s] for s in range(sections)]
    depth = delay[-1]

    condition = conditions(guide_bin, time_step, guide_table)[:, 0]
    modulation = (condition + section_table[0].reshape(-1)).reshape(batches, 3, width)
    value_weight = value_weight[0]
    proj_weight = proj_weight[0]
    edge_in = inputs.reshape(units, rows, width)
    edge_grad = out_grad.reshape(units, rows, width)
    late = (place >= far).astype(jnp.int32)
    info = jnp.stack([place, place + late, sections - 1 - place + 1 - late]).astype(jnp.int32)
    core = lax.axis_index(DP[2]).astype(jnp.int32).reshape(1)
    turns = [
        [(lax.axis_index(axis) + step) % lax.axis_size(axis) for step in range(lax.axis_size(axis))]
        for axis in DP[:2]
    ]
    info, core, (outer_turns, inner_turns) = lax.optimization_barrier((info, core, turns))

    vmem = pl.BlockSpec(memory_space=pltpu.VMEM)
    smem = pl.BlockSpec(memory_space=pltpu.SMEM)
    value_weight, proj_weight, edge_in, edge_grad = (
        pltpu.with_memory_space_constraint(value, pltpu.VMEM)
        for value in (value_weight, proj_weight, edge_in, edge_grad)
    )

    def slots_of(dtype):
        return jax.ShapeDtypeStruct((units, rows, width), dtype)

    flops = 4 * rows * width * value_width
    cost = pl.CostEstimate(flops=flops, bytes_accessed=16 * rows * width, transcendentals=0)
    params = pltpu.CompilerParams(vmem_limit_bytes=10 * 1024 * 1024)
    hop = jax.ShapeDtypeStruct((rows, width), jnp.bfloat16)

    def forward(tick, direct, distant, kept):
        extra = [value for value in (direct, distant) if value is not None]
        operands = (info, edge_in, *extra, modulation, value_weight, proj_weight, *kept)
        lead = len(operands) - len(kept)
        return pl.pallas_call(
            functools.partial(
                forward_kernel, tick, units, direct is not None, distant is not None, far
            ),
            in_specs=[smem] + [vmem] * (len(operands) - 1),
            out_specs=[vmem] * 5,
            out_shape=[hop]
            + [slots_of(dtype) for dtype in (jnp.bfloat16, jnp.bfloat16, jnp.bfloat16, jnp.float32)],
            input_output_aliases={lead + i: 1 + i for i in range(len(kept))},
            cost_estimate=cost,
            compiler_params=params,
            name="fwd",
        )(*operands)

    def backward(tick, direct, distant, keep_in, keep_proj, sofar, final=False):
        extra = [value for value in (direct, distant) if value is not None]
        operands = (
            info,
            edge_grad,
            *extra,
            modulation,
            value_weight,
            proj_weight,
            keep_in,
            keep_proj,
            *sofar,
        )
        lead = len(operands) - len(sofar)
        table_shape = jax.ShapeDtypeStruct((3, width), jnp.float32)
        if final:
            out_shape = [slots_of(jnp.bfloat16), table_shape]
            aliases = {lead: 1, lead + 1: 0}
        else:
            out_shape = [hop, *[slots_of(jnp.bfloat16)] * 2, table_shape]
            aliases = {lead: 3, lead + 1: 1, lead + 2: 2} if sofar else {}
        return pl.pallas_call(
            functools.partial(
                backward_kernel,
                tick,
                units,
                direct is not None,
                distant is not None,
                sections - 1,
                far - 1,
                bool(sofar),
                final,
            ),
            in_specs=[smem] + [vmem] * (len(operands) - 1),
            out_specs=[vmem] * len(out_shape),
            out_shape=out_shape,
            input_output_aliases=aliases,
            scratch_shapes=[
                pltpu.VMEM((rows, width), jnp.float32),
                pltpu.VMEM((3, 8, width), jnp.float32),
            ],
            cost_estimate=cost,
            compiler_params=params,
            name="bwd",
        )(*operands)

    def gate(tick, direct, distant, keep_gproj):
        extra = [value for value in (direct, distant) if value is not None]
        operands = (info, edge_grad, *extra, modulation, keep_gproj)
        return pl.pallas_call(
            functools.partial(
                gate_kernel,
                tick,
                units,
                direct is not None,
                distant is not None,
                sections - 1,
                far - 1,
            ),
            in_specs=[smem] + [vmem] * (len(operands) - 1),
            out_specs=vmem,
            out_shape=slots_of(jnp.bfloat16),
            input_output_aliases={len(operands) - 1: 0},
            cost_estimate=pl.CostEstimate(
                flops=rows * width, bytes_accessed=4 * rows * width, transcendentals=0
            ),
            compiler_params=params,
            name="gate",
        )(*operands)

    def send(value, tick, delays, step, is_far):
        pairs, wanted = [], False
        for s in range(sections):
            to = s + step
            if 0 <= to < sections and ((s < far) != (to < far)) == is_far:
                pairs.append((s, to))
                wanted = wanted or 0 <= tick - delays[s] < units
        return lax.ppermute(value, "section", pairs) if wanted else None

    kept, sofar = [], []
    near_f, far_f, near_b, far_b = {}, {}, {}, {}
    last = depth + units - 1
    for tick in range(depth + last):
        if tick <= last:
            block_out, *kept = forward(tick, near_f.get(tick), far_f.get(tick), kept)
            near_f[tick + 1] = send(block_out, tick, delay, 1, False)
            far_f[tick + 2] = send(block_out, tick, delay, 1, True)
        back = tick - depth
        if back >= 0:
            grad_in, *rest = backward(
                back, near_b.get(back), far_b.get(back), kept[0], kept[3], sofar
            )
            sofar = [rest[2], rest[0], rest[1]]
            near_b[back + 1] = send(grad_in, back, back_delay, -1, False)
            far_b[back + 2] = send(grad_in, back, back_delay, -1, True)

    direct, distant = near_b.get(last), far_b.get(last)
    table, keep_gval, keep_gproj = sofar
    keep_gproj = gate(last, direct, distant, keep_gproj)
    halves = split_product(kept[2], keep_gproj, core)
    direct, halves = lax.optimization_barrier((direct, halves))
    keep_gval, table = backward(
        last, direct, distant, kept[0], kept[3], [table, keep_gval, keep_gproj], final=True
    )
    proj_parts, _, _ = scattered(halves, outer_turns, inner_turns, None, None)
    value_parts, proj_parts, table = scattered(
        split_product(kept[1], keep_gval, core), outer_turns, inner_turns, proj_parts, table
    )
    proj_part = summed(*proj_parts)
    value_part = summed(*value_parts)
    table_part = summed_on_arrival(table, DP, 1)
    return (value_part[None], proj_part[None], table_part[None])


def solution(mesh):
    finer = Mesh(
        mesh.devices.reshape(mesh.shape["section"], 4, 4, 2), ("section", "dp_0", "dp_1", "dp_2")
    )
    placed = (
        P(None, DP, None),
        P(None, DP, None),
        P(),
        P(),
        P(),
        P("section", None, None),
        P("section", None, None),
        P("section", None, None),
    )
    return jax.shard_map(
        per_device,
        mesh=finer,
        in_specs=placed,
        out_specs=(P("section", DP, None), P("section", DP, None), P("section", None, DP)),
        check_vma=False,
    )
```

```python
import functools
import math

import jax
import jax.numpy as jnp
from jax import lax
from jax.experimental import pallas as pl
from jax.experimental.pallas import tpu as pltpu
from jax.sharding import Mesh
from jax.sharding import PartitionSpec as P

DP = ("dp_0", "dp_1", "dp_2")

NORM_FLOOR = 0.1
PARTS = 2
CHUNK = 512
PCHUNK = 512
BLOCK = 384
JOINS = 2
BCHUNK = 256
GROUP = 64


def conditions(guide_bin, time_step, guide_table):
    total = guide_table.shape[1]
    half = total // 2
    frequency = jnp.exp(-math.log(10000.0) * jnp.arange(half, dtype=jnp.float32) / half)
    angle = time_step.astype(jnp.float32)[..., None] * frequency
    waves = jnp.concatenate([jnp.sin(angle), jnp.cos(angle)], axis=-1)
    bin_count = guide_table.shape[0]
    onehot = (guide_bin[..., None] == jnp.arange(bin_count, dtype=jnp.int32)).astype(jnp.float32)
    picked = jnp.einsum(
        "msb,bw->msw", onehot, guide_table.astype(jnp.float32), precision=lax.Precision.HIGHEST
    )
    return picked + 0.5 * waves


def row_mean(value):
    return jnp.sum(value, axis=-1, keepdims=True) * (1.0 / value.shape[-1])


def normalize(hidden):
    centre = row_mean(hidden)
    centred = hidden - centre
    inverse = lax.rsqrt(row_mean(centred * centred) + NORM_FLOOR)
    return (centred * inverse, inverse)


def chosen_input(place, unit, at, edge, direct, far, first_at, far_at):
    value = edge[unit, at, :]
    if direct is not None:
        value = jnp.where(place == first_at, value, direct[at, :])
    return value if far is None else jnp.where(place == far_at, far[at, :], value)


def row_groups(rows, body):
    def step(index, carry):
        body(pl.ds(pl.multiple_of(index * GROUP, GROUP), GROUP))
        return carry

    lax.fori_loop(0, rows // GROUP, step, 0)


def column_chunks(columns, body):
    def step(index, carry):
        body(pl.ds(pl.multiple_of(index * CHUNK, CHUNK), CHUNK))
        return carry

    lax.fori_loop(0, columns // CHUNK, step, 0)


def forward_kernel(tick, units, has_direct, has_far, far_at, joined, *refs):
    info, edge = refs[0], refs[1]
    rest = list(refs[2:])
    direct = rest.pop(0) if has_direct else None
    far = rest.pop(0) if has_far else None
    mod, weight = rest[0], rest[1]
    if joined:
        block_out, keep_in, keep_mod, keep_proj = rest[-4:]
    else:
        proj_weight = rest[2]
        block_out, keep_in, keep_mod, keep_proj, values = rest[-5:]
    unit = tick - info[1]
    batch = lax.div(unit, PARTS)

    @pl.when((unit >= 0) & (unit < units))
    def _():
        def modulate(at):
            block_in = chosen_input(info[0], unit, at, edge, direct, far, 0, far_at)
            keep_in[unit, at, :] = block_in
            normed, _ = normalize(block_in.astype(jnp.float32))
            shift, scale = mod[batch, 0:1, :], mod[batch, 1:2, :]
            keep_mod[unit, at, :] = (normed * (1.0 + scale) + shift).astype(jnp.bfloat16)

        row_groups(block_out.shape[0], modulate)

        def first(at):
            values[:, at] = jnp.dot(
                keep_mod[unit], weight[:, at], preferred_element_type=jnp.float32
            ).astype(jnp.bfloat16)

        if not joined:
            column_chunks(weight.shape[1], first)

        def second(at):
            if joined:
                left, right = keep_mod[unit], weight[:, at]
            else:
                left, right = values[...], proj_weight[:, at]
            projected = jnp.dot(left, right, preferred_element_type=jnp.float32)
            keep_proj[unit, :, at] = projected
            hidden = keep_in[unit, :, at].astype(jnp.float32)
            block_out[:, at] = (hidden + mod[batch, 2:3, at] * projected).astype(jnp.bfloat16)

        column_chunks(block_out.shape[1], second)


def join_kernel(part, value_weight, proj_weight, *refs):
    joined = refs[-1]
    chunks = joined.shape[1] // PCHUNK
    start = part * (joined.shape[0] // JOINS)

    def block(step, carry):
        down = pl.ds(pl.multiple_of(start + lax.div(step, chunks) * BLOCK, BLOCK), BLOCK)
        at = pl.ds(pl.multiple_of(lax.rem(step, chunks) * PCHUNK, PCHUNK), PCHUNK)
        joined[down, at] = jnp.dot(
            value_weight[down, :], proj_weight[:, at], preferred_element_type=jnp.float32
        ).astype(jnp.bfloat16)
        return carry

    lax.fori_loop(0, joined.shape[0] // JOINS // BLOCK * chunks, block, 0)


def batch_kernel(transposed, left, weight, out):
    units, rows, depth = left.shape

    def chunk(at):
        flat = left[...].reshape(units * rows, depth)
        if transposed:
            total = lax.dot_general(
                flat, weight[at, :], (((1,), (1,)), ((), ())), preferred_element_type=jnp.float32
            )
        else:
            total = jnp.dot(flat, weight[:, at], preferred_element_type=jnp.float32)
        out[:, :, at] = total.astype(jnp.bfloat16).reshape(units, rows, total.shape[1])

    def step(index, carry):
        chunk(pl.ds(pl.multiple_of(index * BCHUNK, BCHUNK), BCHUNK))
        return carry

    lax.fori_loop(0, out.shape[2] // BCHUNK, step, 0)


def gate_kernel(tick, units, has_direct, has_far, first_at, far_at, *refs):
    info, edge = refs[0], refs[1]
    rest = list(refs[2:])
    direct = rest.pop(0) if has_direct else None
    far = rest.pop(0) if has_far else None
    mod, keep_gproj = rest[0], rest[-1]
    unit = tick - info[2]

    @pl.when((unit >= 0) & (unit < units))
    def _():
        def gated(at):
            upstream = chosen_input(info[0], unit, at, edge, direct, far, first_at, far_at)
            keep_gproj[unit, at, :] = (
                mod[lax.div(unit, PARTS), 2:3, :] * upstream.astype(jnp.float32)
            ).astype(jnp.bfloat16)

        row_groups(keep_gproj.shape[1], gated)


def backward_kernel(
    tick, units, has_direct, has_far, first_at, far_at, has_table, final, *refs
):
    info, edge = refs[0], refs[1]
    rest = list(refs[2:])
    direct = rest.pop(0) if has_direct else None
    far = rest.pop(0) if has_far else None
    mod, joined, keep_in, keep_proj = rest[:4]
    table_in = rest[4] if has_table else None
    grad_mod, sums = rest[-2:]
    if final:
        keep_gproj, proj_weight = rest[5], rest[7]
        keep_gval, table_out = rest[-4:-2]
    else:
        grad_in, keep_gproj, table_out = rest[-5:-2]
    unit = tick - info[2]
    batch = lax.div(unit, PARTS)
    valid = (unit >= 0) & (unit < units)
    rows, width = grad_mod.shape

    @pl.when(jnp.logical_not(valid))
    def _():
        table_out[...] = jnp.zeros_like(table_out) if table_in is None else table_in[...]

    @pl.when(valid)
    def _():
        def upstream(at):
            return chosen_input(info[0], unit, at, edge, direct, far, first_at, far_at).astype(
                jnp.float32
            )

        def gated(at):
            keep_gproj[unit, at, :] = (mod[batch, 2:3, :] * upstream(at)).astype(jnp.bfloat16)

        if not final:
            row_groups(rows, gated)
        transposed = (((1,), (1,)), ((), ()))

        def first(at):
            keep_gval[unit, :, at] = lax.dot_general(
                keep_gproj[unit], proj_weight[at, :], transposed, preferred_element_type=jnp.float32
            ).astype(jnp.bfloat16)

        if final:
            column_chunks(proj_weight.shape[0], first)

        def second(at):
            grad_mod[:, at] = lax.dot_general(
                keep_gproj[unit], joined[at, :], transposed, preferred_element_type=jnp.float32
            )

        column_chunks(joined.shape[0], second)
        sums[...] = jnp.zeros_like(sums)

        def finish(at):
            normed, inverse = normalize(keep_in[unit, at, :].astype(jnp.float32))
            grad, grad_up = grad_mod[at, :], upstream(at)
            for index, term in enumerate((grad, grad * normed, grad_up * keep_proj[unit, at, :])):
                sums[index] += jnp.sum(term.reshape(GROUP // 8, 8, width), axis=0)
            if final:
                return
            grad_norm = grad * (1.0 + mod[batch, 1:2, :])
            centre_grad = row_mean(grad_norm)
            cross = row_mean(grad_norm * normed)
            grad_in[at, :] = (
                grad_up + inverse * (grad_norm - centre_grad - normed * cross)
            ).astype(jnp.bfloat16)

        row_groups(rows, finish)
        for index in range(3):
            total = jnp.sum(sums[index], axis=0, keepdims=True)
            table_out[index : index + 1, :] = (
                total if table_in is None else table_in[index : index + 1, :] + total
            )


def product_kernel(core, left, right, leaving, staying, tall):
    depth = left.shape[0] * left.shape[1]
    rows = leaving.shape[1]
    tall[...] = jnp.transpose(left[...].reshape(depth, left.shape[2]))
    pairs = BLOCK // (2 * rows)
    chunks = right.shape[2] // PCHUNK

    def block(step, carry):
        down = lax.div(step, chunks)
        at = pl.ds(pl.multiple_of(lax.rem(step, chunks) * PCHUNK, PCHUNK), PCHUNK)
        total = jnp.dot(
            tall[pl.ds(pl.multiple_of(down * BLOCK, BLOCK), BLOCK), :],
            right[:, :, at].reshape(depth, PCHUNK),
            preferred_element_type=jnp.float32,
        ).astype(jnp.bfloat16)
        for pair in range(pairs):
            even = total[(2 * pair) * rows : (2 * pair + 1) * rows]
            odd = total[(2 * pair + 1) * rows : (2 * pair + 2) * rows]
            group = down * pairs + pair
            staying[group, :, at] = jnp.where(core[0] == 0, even, odd)
            leaving[group, :, at] = jnp.where(core[0] == 0, odd, even)
        return carry

    lax.fori_loop(0, tall.shape[0] // BLOCK * chunks, block, 0)


def split_product(left, right, core):
    outer, inner, cores = (lax.axis_size(axis) for axis in DP)
    units, unit_rows, width = right.shape
    rows = left.shape[2] // (outer * inner * cores)
    whole = jax.ShapeDtypeStruct((outer * inner, rows, width), jnp.bfloat16)
    vmem = pl.BlockSpec(memory_space=pltpu.VMEM)
    return pl.pallas_call(
        product_kernel,
        in_specs=[pl.BlockSpec(memory_space=pltpu.SMEM), vmem, vmem],
        out_specs=[vmem, vmem],
        out_shape=[whole, whole],
        scratch_shapes=[pltpu.VMEM((left.shape[2], units * unit_rows), jnp.bfloat16)],
        cost_estimate=pl.CostEstimate(
            flops=2 * units * unit_rows * left.shape[2] * width,
            bytes_accessed=2 * left.shape[2] * width,
            transcendentals=0,
        ),
        compiler_params=pltpu.CompilerParams(vmem_limit_bytes=12 * 1024 * 1024),
        name="product",
    )(core, left, right)


def taken(parts, index):
    return lax.dynamic_index_in_dim(parts, index, 0, keepdims=False)


def summed(*parts):
    total = parts[0].astype(jnp.float32)
    for part in parts[1:]:
        total = total + part.astype(jnp.float32)
    return total


def turned(value, axis, step):
    peers = lax.axis_size(axis)
    return lax.ppermute(value, axis, [(i, (i + step) % peers) for i in range(peers)])


def swapped_sum(leaving, staying):
    arrived = lax.ppermute(leaving, DP[2], [(0, 1), (1, 0)])
    return summed(staying, arrived).astype(jnp.bfloat16)


def ring_parts(parts, turns):
    middle = parts.shape[1] // 2
    across = taken(parts, turns[2])
    above = turned(across[:middle], DP[0], 1)
    below = turned(across[middle:], DP[0], -1)
    ahead, behind = taken(parts, turns[1]), taken(parts, turns[3])
    ahead = jnp.concatenate(
        [summed(ahead[:middle], above).astype(jnp.bfloat16), ahead[middle:]], axis=0
    )
    behind = jnp.concatenate(
        [behind[:middle], summed(behind[middle:], below).astype(jnp.bfloat16)], axis=0
    )
    return [taken(parts, turns[0]), turned(ahead, DP[0], 1), turned(behind, DP[0], -1)]


def sent_around(parts, turns, leaving):
    arrived = [turned(part, DP[1], step) for step, part in enumerate(leaving, 1)]
    return [taken(parts, turns[0]), *arrived]


def scattered(halves, outer_turns, inner_turns, ahead, table):
    outer, inner = (lax.axis_size(axis) for axis in DP[:2])
    parts = swapped_sum(*halves)
    rows, width = parts.shape[1:]
    parts = ring_parts(parts.reshape(outer, inner * rows, width), outer_turns)
    if ahead is not None:
        parts, ahead = lax.optimization_barrier((parts, ahead))
    parts = summed(*parts).astype(jnp.bfloat16).reshape(inner, rows, width)
    leaving = [taken(parts, turn) for turn in inner_turns[1:]]
    if table is not None:
        leaving, table = lax.optimization_barrier((leaving, table))
    return sent_around(parts, inner_turns, leaving), ahead, table


def summed_on_arrival(value, axis, dim):
    peers = lax.axis_size(axis)
    dims = value.shape
    parts = value.reshape(*dims[:dim], peers, dims[dim] // peers, *dims[dim + 1 :])
    parts = jnp.moveaxis(parts, dim, 0)
    arrived = lax.all_to_all(parts, axis, split_axis=0, concat_axis=0, tiled=True)
    return arrived.sum(axis=0)


def per_device(
    inputs, out_grad, guide_bin, time_step, guide_table, section_table, value_weight, proj_weight
):
    sections = lax.axis_size("section")
    place = lax.axis_index("section")
    batches, tok_dev, width = inputs.shape
    value_width = value_weight.shape[2]
    rows = tok_dev // PARTS
    units = batches * PARTS
    far = sections // 2
    delay = [s + (s >= far) for s in range(sections)]
    back_delay = [delay[sections - 1 - s] for s in range(sections)]
    depth = delay[-1]

    condition = conditions(guide_bin, time_step, guide_table)[:, 0]
    modulation = (condition + section_table[0].reshape(-1)).reshape(batches, 3, width)
    value_weight = value_weight[0]
    proj_weight = proj_weight[0]
    edge_in = inputs.reshape(units, rows, width)
    edge_grad = out_grad.reshape(units, rows, width)
    late = (place >= far).astype(jnp.int32)
    info = jnp.stack([place, place + late, sections - 1 - place + 1 - late]).astype(jnp.int32)
    core = lax.axis_index(DP[2]).astype(jnp.int32).reshape(1)
    turns = [
        [(lax.axis_index(axis) + step) % lax.axis_size(axis) for step in range(lax.axis_size(axis))]
        for axis in DP[:2]
    ]
    info, core, (outer_turns, inner_turns) = lax.optimization_barrier((info, core, turns))

    vmem = pl.BlockSpec(memory_space=pltpu.VMEM)
    smem = pl.BlockSpec(memory_space=pltpu.SMEM)
    value_weight, proj_weight, edge_in, edge_grad = (
        pltpu.with_memory_space_constraint(value, pltpu.VMEM)
        for value in (value_weight, proj_weight, edge_in, edge_grad)
    )

    def slots_of(dtype):
        return jax.ShapeDtypeStruct((units, rows, width), dtype)

    flops = 2 * rows * width * value_width
    cost = pl.CostEstimate(flops=flops, bytes_accessed=16 * rows * width, transcendentals=0)
    params = pltpu.CompilerParams(vmem_limit_bytes=10 * 1024 * 1024)
    hop = jax.ShapeDtypeStruct((rows, width), jnp.bfloat16)

    def forward(tick, direct, distant, kept, weights):
        extra = [value for value in (direct, distant) if value is not None]
        operands = (info, edge_in, *extra, modulation, *weights, *kept)
        lead = len(operands) - len(kept)
        joined = len(weights) == 1
        return pl.pallas_call(
            functools.partial(
                forward_kernel, tick, units, direct is not None, distant is not None, far, joined
            ),
            in_specs=[smem] + [vmem] * (len(operands) - 1),
            out_specs=[vmem] * 4,
            out_shape=[hop]
            + [slots_of(dtype) for dtype in (jnp.bfloat16, jnp.bfloat16, jnp.float32)],
            input_output_aliases={lead + i: 1 + i for i in range(len(kept))},
            scratch_shapes=[] if joined else [pltpu.VMEM((rows, value_width), jnp.bfloat16)],
            cost_estimate=cost,
            compiler_params=params,
            name="fwd",
        )(*operands)

    def join(part, sofar):
        return pl.pallas_call(
            functools.partial(join_kernel, part),
            in_specs=[vmem] * (2 + len(sofar)),
            out_specs=vmem,
            out_shape=jax.ShapeDtypeStruct((width, width), jnp.bfloat16),
            input_output_aliases={2: 0} if sofar else {},
            cost_estimate=pl.CostEstimate(
                flops=2 * width * width * value_width // JOINS,
                bytes_accessed=6 * width * width,
                transcendentals=0,
            ),
            compiler_params=params,
            name="join",
        )(value_weight, proj_weight, *sofar)

    def batch_product(left, weight, transposed):
        return pl.pallas_call(
            functools.partial(batch_kernel, transposed),
            in_specs=[vmem] * 2,
            out_specs=vmem,
            out_shape=slots_of(jnp.bfloat16),
            cost_estimate=pl.CostEstimate(
                flops=2 * units * rows * width * value_width,
                bytes_accessed=2 * width * width,
                transcendentals=0,
            ),
            compiler_params=params,
            name="batch",
        )(left, weight)

    def backward(tick, direct, distant, keep_in, keep_proj, sofar, final=False):
        extra = [value for value in (direct, distant) if value is not None]
        operands = (info, edge_grad, *extra, modulation, joined, keep_in, keep_proj, *sofar)
        lead = 2 + len(extra) + 4
        table_shape = jax.ShapeDtypeStruct((3, width), jnp.float32)
        if final:
            out_shape = [slots_of(jnp.bfloat16), table_shape]
            aliases = {lead: 1, lead + 2: 0}
        else:
            out_shape = [hop, slots_of(jnp.bfloat16), table_shape]
            aliases = {lead: 2, lead + 1: 1} if sofar else {}
        return pl.pallas_call(
            functools.partial(
                backward_kernel,
                tick,
                units,
                direct is not None,
                distant is not None,
                sections - 1,
                far - 1,
                bool(sofar),
                final,
            ),
            in_specs=[smem] + [vmem] * (len(operands) - 1),
            out_specs=[vmem] * len(out_shape),
            out_shape=out_shape,
            input_output_aliases=aliases,
            scratch_shapes=[
                pltpu.VMEM((rows, width), jnp.float32),
                pltpu.VMEM((3, 8, width), jnp.float32),
            ],
            cost_estimate=cost,
            compiler_params=params,
            name="bwd",
        )(*operands)

    def gate(tick, direct, distant, keep_gproj):
        extra = [value for value in (direct, distant) if value is not None]
        operands = (info, edge_grad, *extra, modulation, keep_gproj)
        return pl.pallas_call(
            functools.partial(
                gate_kernel,
                tick,
                units,
                direct is not None,
                distant is not None,
                sections - 1,
                far - 1,
            ),
            in_specs=[smem] + [vmem] * (len(operands) - 1),
            out_specs=vmem,
            out_shape=slots_of(jnp.bfloat16),
            input_output_aliases={len(operands) - 1: 0},
            cost_estimate=pl.CostEstimate(
                flops=rows * width, bytes_accessed=4 * rows * width, transcendentals=0
            ),
            compiler_params=params,
            name="gate",
        )(*operands)

    def send(value, tick, delays, step, is_far):
        pairs, wanted = [], False
        for s in range(sections):
            to = s + step
            if 0 <= to < sections and ((s < far) != (to < far)) == is_far:
                pairs.append((s, to))
                wanted = wanted or 0 <= tick - delays[s] < units
        return lax.ppermute(value, "section", pairs) if wanted else None

    kept, sofar, join_parts = [], [], []
    near_f, far_f, near_b, far_b = {}, {}, {}, {}
    last = depth + units - 1
    for tick in range(depth + last):
        if tick <= last:
            weights = [value_weight, proj_weight] if tick < JOINS else [joined]
            block_out, *kept = forward(tick, near_f.get(tick), far_f.get(tick), kept, weights)
            if tick < JOINS:
                block_out, value_weight, join_parts = lax.optimization_barrier(
                    (block_out, value_weight, join_parts)
                )
                joined = join(tick, join_parts)
                join_parts = [joined]
            near_f[tick + 1] = send(block_out, tick, delay, 1, False)
            far_f[tick + 2] = send(block_out, tick, delay, 1, True)
        back = tick - depth
        if back >= 0:
            grad_in, *rest = backward(
                back, near_b.get(back), far_b.get(back), kept[0], kept[2], sofar
            )
            sofar = [rest[1], rest[0]]
            if back == last - 4:
                grad_in, keep_mod = lax.optimization_barrier((grad_in, kept[1]))
                keep_val = batch_product(keep_mod, value_weight, False)
            if back == last - 1:
                grad_in, sofar = lax.optimization_barrier((grad_in, sofar))
                keep_gval = batch_product(sofar[1], proj_weight, True)
            near_b[back + 1] = send(grad_in, back, back_delay, -1, False)
            far_b[back + 2] = send(grad_in, back, back_delay, -1, True)

    direct, distant = near_b.get(last), far_b.get(last)
    table, keep_gproj = sofar
    direct, keep_gproj, keep_gval = lax.optimization_barrier((direct, keep_gproj, keep_gval))
    keep_gproj = gate(last, direct, distant, keep_gproj)
    halves = split_product(keep_val, keep_gproj, core)
    direct, halves = lax.optimization_barrier((direct, halves))
    keep_gval, table = backward(
        last,
        direct,
        distant,
        kept[0],
        kept[2],
        [table, keep_gproj, keep_gval, proj_weight],
        final=True,
    )
    proj_parts, _, _ = scattered(halves, outer_turns, inner_turns, None, None)
    value_parts, proj_parts, table = scattered(
        split_product(keep_mod, keep_gval, core), outer_turns, inner_turns, proj_parts, table
    )
    proj_part = summed(*proj_parts)
    value_part = summed(*value_parts)
    table_part = summed_on_arrival(table, DP, 1)
    return (value_part[None], proj_part[None], table_part[None])


def solution(mesh):
    finer = Mesh(
        mesh.devices.reshape(mesh.shape["section"], 4, 4, 2), ("section", "dp_0", "dp_1", "dp_2")
    )
    placed = (
        P(None, DP, None),
        P(None, DP, None),
        P(),
        P(),
        P(),
        P("section", None, None),
        P("section", None, None),
        P("section", None, None),
    )
    return jax.shard_map(
        per_device,
        mesh=finer,
        in_specs=placed,
        out_specs=(P("section", DP, None), P("section", DP, None), P("section", None, DP)),
        check_vma=False,
    )
```

```python
import functools
import math

import jax
import jax.numpy as jnp
from jax import lax
from jax.experimental import pallas as pl
from jax.experimental.pallas import tpu as pltpu
from jax.sharding import Mesh
from jax.sharding import PartitionSpec as P

DP = ("dp_0", "dp_1", "dp_2")

NORM_FLOOR = 0.1
PARTS = 2
CHUNK = 512
PCHUNK = 512
BLOCK = 384
TALL = 768
JOINS = 2
BCHUNK = 256
GROUP = 64


def conditions(guide_bin, time_step, guide_table):
    total = guide_table.shape[1]
    half = total // 2
    frequency = jnp.exp(-math.log(10000.0) * jnp.arange(half, dtype=jnp.float32) / half)
    angle = time_step.astype(jnp.float32)[..., None] * frequency
    waves = jnp.concatenate([jnp.sin(angle), jnp.cos(angle)], axis=-1)
    bin_count = guide_table.shape[0]
    onehot = (guide_bin[..., None] == jnp.arange(bin_count, dtype=jnp.int32)).astype(jnp.float32)
    picked = jnp.einsum(
        "msb,bw->msw", onehot, guide_table.astype(jnp.float32), precision=lax.Precision.HIGHEST
    )
    return picked + 0.5 * waves


def row_mean(value):
    return jnp.sum(value, axis=-1, keepdims=True) * (1.0 / value.shape[-1])


def normalize(hidden):
    centre = row_mean(hidden)
    centred = hidden - centre
    inverse = lax.rsqrt(row_mean(centred * centred) + NORM_FLOOR)
    return (centred * inverse, inverse)


def chosen_input(place, unit, at, edge, direct, far, first_at, far_at):
    value = edge[unit, at, :]
    if direct is not None:
        value = jnp.where(place == first_at, value, direct[at, :])
    return value if far is None else jnp.where(place == far_at, far[at, :], value)


def row_groups(rows, body):
    def step(index, carry):
        body(pl.ds(pl.multiple_of(index * GROUP, GROUP), GROUP))
        return carry

    lax.fori_loop(0, rows // GROUP, step, 0)


def column_chunks(columns, body):
    def step(index, carry):
        body(pl.ds(pl.multiple_of(index * CHUNK, CHUNK), CHUNK))
        return carry

    lax.fori_loop(0, columns // CHUNK, step, 0)


def forward_kernel(tick, units, has_direct, has_far, far_at, joined, *refs):
    info, edge = refs[0], refs[1]
    rest = list(refs[2:])
    direct = rest.pop(0) if has_direct else None
    far = rest.pop(0) if has_far else None
    mod, weight = rest[0], rest[1]
    if joined:
        block_out, keep_in, keep_mod, keep_proj = rest[-4:]
    else:
        proj_weight = rest[2]
        block_out, keep_in, keep_mod, keep_proj, values = rest[-5:]
    unit = tick - info[1]
    batch = lax.div(unit, PARTS)

    @pl.when((unit >= 0) & (unit < units))
    def _():
        def modulate(at):
            block_in = chosen_input(info[0], unit, at, edge, direct, far, 0, far_at)
            keep_in[unit, at, :] = block_in
            normed, _ = normalize(block_in.astype(jnp.float32))
            shift, scale = mod[batch, 0:1, :], mod[batch, 1:2, :]
            keep_mod[unit, at, :] = (normed * (1.0 + scale) + shift).astype(jnp.bfloat16)

        row_groups(block_out.shape[0], modulate)

        def first(at):
            values[:, at] = jnp.dot(
                keep_mod[unit], weight[:, at], preferred_element_type=jnp.float32
            ).astype(jnp.bfloat16)

        if not joined:
            column_chunks(weight.shape[1], first)

        def second(at):
            if joined:
                left, right = keep_mod[unit], weight[:, at]
            else:
                left, right = values[...], proj_weight[:, at]
            projected = jnp.dot(left, right, preferred_element_type=jnp.float32)
            keep_proj[unit, :, at] = projected
            hidden = keep_in[unit, :, at].astype(jnp.float32)
            block_out[:, at] = (hidden + mod[batch, 2:3, at] * projected).astype(jnp.bfloat16)

        column_chunks(block_out.shape[1], second)


def join_kernel(part, value_weight, proj_weight, *refs):
    joined = refs[-1]
    chunks = joined.shape[1] // PCHUNK
    start = part * (joined.shape[0] // JOINS)

    def block(step, carry):
        down = pl.ds(pl.multiple_of(start + lax.div(step, chunks) * BLOCK, BLOCK), BLOCK)
        at = pl.ds(pl.multiple_of(lax.rem(step, chunks) * PCHUNK, PCHUNK), PCHUNK)
        joined[down, at] = jnp.dot(
            value_weight[down, :], proj_weight[:, at], preferred_element_type=jnp.float32
        ).astype(jnp.bfloat16)
        return carry

    lax.fori_loop(0, joined.shape[0] // JOINS // BLOCK * chunks, block, 0)


def batch_kernel(transposed, upright, left, weight, out):
    units, rows, depth = left.shape

    def chunk(at):
        flat = left[...].reshape(units * rows, depth)
        if transposed:
            total = lax.dot_general(
                flat, weight[at, :], (((1,), (1,)), ((), ())), preferred_element_type=jnp.float32
            )
        else:
            total = jnp.dot(flat, weight[:, at], preferred_element_type=jnp.float32)
        total = total.astype(jnp.bfloat16)
        if upright:
            out[at, :] = jnp.transpose(total)
        else:
            out[:, :, at] = total.reshape(units, rows, total.shape[1])

    def step(index, carry):
        chunk(pl.ds(pl.multiple_of(index * BCHUNK, BCHUNK), BCHUNK))
        return carry

    lax.fori_loop(0, weight.shape[0] // BCHUNK, step, 0)


def gate_kernel(tick, units, has_direct, has_far, first_at, far_at, *refs):
    info, edge = refs[0], refs[1]
    rest = list(refs[2:])
    direct = rest.pop(0) if has_direct else None
    far = rest.pop(0) if has_far else None
    mod, keep_gproj = rest[0], rest[-1]
    unit = tick - info[2]

    @pl.when((unit >= 0) & (unit < units))
    def _():
        def gated(at):
            upstream = chosen_input(info[0], unit, at, edge, direct, far, first_at, far_at)
            keep_gproj[unit, at, :] = (
                mod[lax.div(unit, PARTS), 2:3, :] * upstream.astype(jnp.float32)
            ).astype(jnp.bfloat16)

        row_groups(keep_gproj.shape[1], gated)


def value_kernel(tick, units, info, keep_gproj, proj_weight, keep_gval_in, keep_gval):
    unit = tick - info[2]

    @pl.when((unit >= 0) & (unit < units))
    def _():
        def chunk(at):
            keep_gval[unit, :, at] = lax.dot_general(
                keep_gproj[unit],
                proj_weight[at, :],
                (((1,), (1,)), ((), ())),
                preferred_element_type=jnp.float32,
            ).astype(jnp.bfloat16)

        column_chunks(proj_weight.shape[0], chunk)


def backward_kernel(
    tick, units, has_direct, has_far, first_at, far_at, has_table, final, *refs
):
    info, edge = refs[0], refs[1]
    rest = list(refs[2:])
    direct = rest.pop(0) if has_direct else None
    far = rest.pop(0) if has_far else None
    mod, joined, keep_in, keep_proj = rest[:4]
    table_in = rest[4] if has_table else None
    grad_mod, sums = rest[-2:]
    if final:
        keep_gproj, table_out = rest[5], rest[-3]
    else:
        grad_in, keep_gproj, table_out = rest[-5:-2]
    unit = tick - info[2]
    batch = lax.div(unit, PARTS)
    valid = (unit >= 0) & (unit < units)
    rows, width = grad_mod.shape

    @pl.when(jnp.logical_not(valid))
    def _():
        table_out[...] = jnp.zeros_like(table_out) if table_in is None else table_in[...]

    @pl.when(valid)
    def _():
        def upstream(at):
            return chosen_input(info[0], unit, at, edge, direct, far, first_at, far_at).astype(
                jnp.float32
            )

        def gated(at):
            keep_gproj[unit, at, :] = (mod[batch, 2:3, :] * upstream(at)).astype(jnp.bfloat16)

        if not final:
            row_groups(rows, gated)
        transposed = (((1,), (1,)), ((), ()))

        def second(at):
            grad_mod[:, at] = lax.dot_general(
                keep_gproj[unit], joined[at, :], transposed, preferred_element_type=jnp.float32
            )

        column_chunks(joined.shape[0], second)
        sums[...] = jnp.zeros_like(sums)

        def finish(at):
            normed, inverse = normalize(keep_in[unit, at, :].astype(jnp.float32))
            grad, grad_up = grad_mod[at, :], upstream(at)
            for index, term in enumerate((grad, grad * normed, grad_up * keep_proj[unit, at, :])):
                sums[index] += jnp.sum(term.reshape(GROUP // 8, 8, width), axis=0)
            if final:
                return
            grad_norm = grad * (1.0 + mod[batch, 1:2, :])
            centre_grad = row_mean(grad_norm)
            cross = row_mean(grad_norm * normed)
            grad_in[at, :] = (
                grad_up + inverse * (grad_norm - centre_grad - normed * cross)
            ).astype(jnp.bfloat16)

        row_groups(rows, finish)
        for index in range(3):
            total = jnp.sum(sums[index], axis=0, keepdims=True)
            table_out[index : index + 1, :] = (
                total if table_in is None else table_in[index : index + 1, :] + total
            )


def product_kernel(core, tall, right, leaving, staying):
    depth = tall.shape[1]
    rows = leaving.shape[1]
    pairs = TALL // (2 * rows)
    chunks = right.shape[2] // PCHUNK

    def block(step, carry):
        down = lax.div(step, chunks)
        at = pl.ds(pl.multiple_of(lax.rem(step, chunks) * PCHUNK, PCHUNK), PCHUNK)
        total = jnp.dot(
            tall[pl.ds(pl.multiple_of(down * TALL, TALL), TALL), :],
            right[:, :, at].reshape(depth, PCHUNK),
            preferred_element_type=jnp.float32,
        ).astype(jnp.bfloat16)
        for pair in range(pairs):
            even = total[(2 * pair) * rows : (2 * pair + 1) * rows]
            odd = total[(2 * pair + 1) * rows : (2 * pair + 2) * rows]
            group = down * pairs + pair
            staying[group, :, at] = jnp.where(core[0] == 0, even, odd)
            leaving[group, :, at] = jnp.where(core[0] == 0, odd, even)
        return carry

    lax.fori_loop(0, tall.shape[0] // TALL * chunks, block, 0)


def turn_kernel(left, tall):
    depth = left.shape[0] * left.shape[1]

    def chunk(at):
        tall[at, :] = jnp.transpose(left[:, :, at].reshape(depth, CHUNK))

    column_chunks(left.shape[2], chunk)


def open_kernel(turns, staying, arrived, own, ahead, behind, top, bottom):
    inner = own.shape[0]
    half = inner // 2

    def added(turn, index):
        at = turns[turn] * inner + index
        return (staying[at].astype(jnp.float32) + arrived[at].astype(jnp.float32)).astype(
            jnp.bfloat16
        )

    def step(index, carry):
        own[index] = added(0, index)
        ahead[index] = added(1, index)
        behind[index] = added(3, index)
        return carry

    lax.fori_loop(0, inner, step, 0)

    def halves(index, carry):
        top[index] = added(2, index)
        bottom[index] = added(2, index + half)
        return carry

    lax.fori_loop(0, half, halves, 0)


def relay_kernel(ahead, behind, above, below, ahead_out, behind_out):
    half = above.shape[0]

    def step(index, carry):
        ahead_out[index] = (
            ahead[index].astype(jnp.float32) + above[index].astype(jnp.float32)
        ).astype(jnp.bfloat16)
        behind_out[index + half] = (
            behind[index + half].astype(jnp.float32) + below[index].astype(jnp.float32)
        ).astype(jnp.bfloat16)
        return carry

    lax.fori_loop(0, half, step, 0)


def split_kernel(turns, own, first, second, *outs):
    for turn, out in enumerate(outs):
        at = turns[turn]
        out[...] = (
            own[at].astype(jnp.float32)
            + first[at].astype(jnp.float32)
            + second[at].astype(jnp.float32)
        ).astype(jnp.bfloat16)


def in_vmem(kernel, name, out_shape, operands, scalars=0, aliases=None, flops=1 << 24):
    smem, vmem = (pl.BlockSpec(memory_space=space) for space in (pltpu.SMEM, pltpu.VMEM))
    return pl.pallas_call(
        kernel,
        in_specs=[smem] * scalars + [vmem] * (len(operands) - scalars),
        out_specs=[vmem] * len(out_shape),
        out_shape=out_shape,
        input_output_aliases=aliases or {},
        cost_estimate=pl.CostEstimate(flops=flops, bytes_accessed=1 << 20, transcendentals=0),
        compiler_params=pltpu.CompilerParams(vmem_limit_bytes=10 * 1024 * 1024),
        name=name,
    )(*operands)


def bf16_of(*dims):
    return jax.ShapeDtypeStruct(dims, jnp.bfloat16)


def split_product(tall, right, core):
    outer, inner, cores = (lax.axis_size(axis) for axis in DP)
    width = right.shape[2]
    whole = bf16_of(outer * inner, tall.shape[0] // (outer * inner * cores), width)
    flops = 2 * tall.shape[0] * tall.shape[1] * width
    return in_vmem(product_kernel, "product", [whole] * 2, (core, tall, right), 1, flops=flops)


def summed(*parts):
    total = parts[0].astype(jnp.float32)
    for part in parts[1:]:
        total = total + part.astype(jnp.float32)
    return total


def turned(value, axis, step):
    peers = lax.axis_size(axis)
    return lax.ppermute(value, axis, [(i, (i + step) % peers) for i in range(peers)])


def opened(halves, turns):
    leaving, staying = halves
    inner = lax.axis_size(DP[1])
    rows, width = leaving.shape[1:]
    arrived = lax.ppermute(leaving, DP[2], [(0, 1), (1, 0)])
    full, half = bf16_of(inner, rows, width), bf16_of(inner // 2, rows, width)
    return in_vmem(
        open_kernel, "open", [full, full, full, half, half], (turns, staying, arrived), 1
    )


def relayed(ahead, behind, top, bottom):
    above, below = turned(top, DP[0], 1), turned(bottom, DP[0], -1)
    shape = bf16_of(*ahead.shape)
    return in_vmem(
        relay_kernel, "relay", [shape] * 2, (ahead, behind, above, below), aliases={0: 0, 1: 1}
    )


def divided(parts, turns):
    shape = bf16_of(*parts[0].shape[1:])
    return in_vmem(split_kernel, "divide", [shape] * parts[0].shape[0], (turns, *parts), 1)


def sent_around(parts):
    return [parts[0]] + [turned(part, DP[1], step) for step, part in enumerate(parts[1:], 1)]


def summed_on_arrival(value, axis, dim):
    peers = lax.axis_size(axis)
    dims = value.shape
    parts = value.reshape(*dims[:dim], peers, dims[dim] // peers, *dims[dim + 1 :])
    parts = jnp.moveaxis(parts, dim, 0)
    arrived = lax.all_to_all(parts, axis, split_axis=0, concat_axis=0, tiled=True)
    return arrived.sum(axis=0)


def per_device(
    inputs, out_grad, guide_bin, time_step, guide_table, section_table, value_weight, proj_weight
):
    sections = lax.axis_size("section")
    place = lax.axis_index("section")
    batches, tok_dev, width = inputs.shape
    value_width = value_weight.shape[2]
    rows = tok_dev // PARTS
    units = batches * PARTS
    far = sections // 2
    delay = [s + (s >= far) for s in range(sections)]
    back_delay = [delay[sections - 1 - s] for s in range(sections)]
    depth = delay[-1]

    condition = conditions(guide_bin, time_step, guide_table)[:, 0]
    modulation = (condition + section_table[0].reshape(-1)).reshape(batches, 3, width)
    value_weight = value_weight[0]
    proj_weight = proj_weight[0]
    edge_in = inputs.reshape(units, rows, width)
    edge_grad = out_grad.reshape(units, rows, width)
    late = (place >= far).astype(jnp.int32)
    info = jnp.stack([place, place + late, sections - 1 - place + 1 - late]).astype(jnp.int32)
    core = lax.axis_index(DP[2]).astype(jnp.int32).reshape(1)
    turns = [
        [(lax.axis_index(axis) + step) % lax.axis_size(axis) for step in range(lax.axis_size(axis))]
        for axis in DP[:2]
    ]
    turns = [jnp.stack(turn).astype(jnp.int32) for turn in turns]
    info, core, (outer_turns, inner_turns) = lax.optimization_barrier((info, core, turns))

    vmem = pl.BlockSpec(memory_space=pltpu.VMEM)
    smem = pl.BlockSpec(memory_space=pltpu.SMEM)
    value_weight, proj_weight, edge_in, edge_grad = (
        pltpu.with_memory_space_constraint(value, pltpu.VMEM)
        for value in (value_weight, proj_weight, edge_in, edge_grad)
    )

    def slots_of(dtype):
        return jax.ShapeDtypeStruct((units, rows, width), dtype)

    flops = 2 * rows * width * value_width
    cost = pl.CostEstimate(flops=flops, bytes_accessed=16 * rows * width, transcendentals=0)
    params = pltpu.CompilerParams(vmem_limit_bytes=10 * 1024 * 1024)
    hop = jax.ShapeDtypeStruct((rows, width), jnp.bfloat16)

    def forward(tick, direct, distant, kept, weights):
        extra = [value for value in (direct, distant) if value is not None]
        operands = (info, edge_in, *extra, modulation, *weights, *kept)
        lead = len(operands) - len(kept)
        joined = len(weights) == 1
        return pl.pallas_call(
            functools.partial(
                forward_kernel, tick, units, direct is not None, distant is not None, far, joined
            ),
            in_specs=[smem] + [vmem] * (len(operands) - 1),
            out_specs=[vmem] * 4,
            out_shape=[hop]
            + [slots_of(dtype) for dtype in (jnp.bfloat16, jnp.bfloat16, jnp.float32)],
            input_output_aliases={lead + i: 1 + i for i in range(len(kept))},
            scratch_shapes=[] if joined else [pltpu.VMEM((rows, value_width), jnp.bfloat16)],
            cost_estimate=cost,
            compiler_params=params,
            name="fwd",
        )(*operands)

    def join(part, sofar):
        return pl.pallas_call(
            functools.partial(join_kernel, part),
            in_specs=[vmem] * (2 + len(sofar)),
            out_specs=vmem,
            out_shape=jax.ShapeDtypeStruct((width, width), jnp.bfloat16),
            input_output_aliases={2: 0} if sofar else {},
            cost_estimate=pl.CostEstimate(
                flops=2 * width * width * value_width // JOINS,
                bytes_accessed=6 * width * width,
                transcendentals=0,
            ),
            compiler_params=params,
            name="join",
        )(value_weight, proj_weight, *sofar)

    def batch_product(left, weight, transposed, upright):
        return pl.pallas_call(
            functools.partial(batch_kernel, transposed, upright),
            in_specs=[vmem] * 2,
            out_specs=vmem,
            out_shape=bf16_of(value_width, units * rows) if upright else slots_of(jnp.bfloat16),
            cost_estimate=pl.CostEstimate(
                flops=2 * units * rows * width * value_width,
                bytes_accessed=2 * width * width,
                transcendentals=0,
            ),
            compiler_params=params,
            name="batch",
        )(left, weight)

    def backward(tick, direct, distant, keep_in, keep_proj, sofar, final=False):
        extra = [value for value in (direct, distant) if value is not None]
        operands = (info, edge_grad, *extra, modulation, joined, keep_in, keep_proj, *sofar)
        lead = 2 + len(extra) + 4
        table_shape = jax.ShapeDtypeStruct((3, width), jnp.float32)
        if final:
            out_shape = [table_shape]
            aliases = {lead: 0}
        else:
            out_shape = [hop, slots_of(jnp.bfloat16), table_shape]
            aliases = {lead: 2, lead + 1: 1} if sofar else {}
        return pl.pallas_call(
            functools.partial(
                backward_kernel,
                tick,
                units,
                direct is not None,
                distant is not None,
                sections - 1,
                far - 1,
                bool(sofar),
                final,
            ),
            in_specs=[smem] + [vmem] * (len(operands) - 1),
            out_specs=[vmem] * len(out_shape),
            out_shape=out_shape,
            input_output_aliases=aliases,
            scratch_shapes=[
                pltpu.VMEM((rows, width), jnp.float32),
                pltpu.VMEM((3, 8, width), jnp.float32),
            ],
            cost_estimate=cost,
            compiler_params=params,
            name="bwd",
        )(*operands)

    def gate(tick, direct, distant, keep_gproj):
        extra = [value for value in (direct, distant) if value is not None]
        operands = (info, edge_grad, *extra, modulation, keep_gproj)
        return pl.pallas_call(
            functools.partial(
                gate_kernel,
                tick,
                units,
                direct is not None,
                distant is not None,
                sections - 1,
                far - 1,
            ),
            in_specs=[smem] + [vmem] * (len(operands) - 1),
            out_specs=vmem,
            out_shape=slots_of(jnp.bfloat16),
            input_output_aliases={len(operands) - 1: 0},
            cost_estimate=pl.CostEstimate(
                flops=rows * width, bytes_accessed=4 * rows * width, transcendentals=0
            ),
            compiler_params=params,
            name="gate",
        )(*operands)

    def send(value, tick, delays, step, is_far):
        pairs, wanted = [], False
        for s in range(sections):
            to = s + step
            if 0 <= to < sections and ((s < far) != (to < far)) == is_far:
                pairs.append((s, to))
                wanted = wanted or 0 <= tick - delays[s] < units
        return lax.ppermute(value, "section", pairs) if wanted else None

    kept, sofar, join_parts = [], [], []
    near_f, far_f, near_b, far_b = {}, {}, {}, {}
    last = depth + units - 1
    for tick in range(depth + last):
        if tick <= last:
            weights = [value_weight, proj_weight] if tick < JOINS else [joined]
            block_out, *kept = forward(tick, near_f.get(tick), far_f.get(tick), kept, weights)
            if tick < JOINS:
                block_out, value_weight, join_parts = lax.optimization_barrier(
                    (block_out, value_weight, join_parts)
                )
                joined = join(tick, join_parts)
                join_parts = [joined]
            near_f[tick + 1] = send(block_out, tick, delay, 1, False)
            far_f[tick + 2] = send(block_out, tick, delay, 1, True)
        back = tick - depth
        if back >= 0:
            grad_in, *rest = backward(
                back, near_b.get(back), far_b.get(back), kept[0], kept[2], sofar
            )
            sofar = [rest[1], rest[0]]
            if back == last - 4:
                grad_in, keep_mod = lax.optimization_barrier((grad_in, kept[1]))
                tall_val = batch_product(keep_mod, value_weight, False, True)
            if back == last - 5:
                grad_in, keep_mod = lax.optimization_barrier((grad_in, kept[1]))
                tall_mod = in_vmem(
                    turn_kernel, "turn", [bf16_of(width, units * rows)], (keep_mod,), flops=1 << 30
                )[0]
            if back == last - 1:
                grad_in, sofar = lax.optimization_barrier((grad_in, sofar))
                keep_gval = batch_product(sofar[1], proj_weight, True, False)
            near_b[back + 1] = send(grad_in, back, back_delay, -1, False)
            far_b[back + 2] = send(grad_in, back, back_delay, -1, True)

    direct, distant = near_b.get(last), far_b.get(last)
    table, keep_gproj = sofar
    direct, keep_gproj, keep_gval = lax.optimization_barrier((direct, keep_gproj, keep_gval))
    keep_gproj = gate(last, direct, distant, keep_gproj)
    proj_halves = split_product(tall_val, keep_gproj, core)
    right, proj_halves = lax.optimization_barrier((keep_gproj, proj_halves))
    keep_gval = in_vmem(
        functools.partial(value_kernel, last, units),
        "value",
        [slots_of(jnp.bfloat16)],
        (info, right, proj_weight, keep_gval),
        1,
        aliases={3: 0},
        flops=flops,
    )[0]
    value_halves = split_product(tall_mod, keep_gval, core)
    proj_open = opened(proj_halves, outer_turns)
    direct, proj_open = lax.optimization_barrier((direct, proj_open))
    table = backward(
        last, direct, distant, kept[0], kept[2], [table, keep_gproj], final=True
    )[0]
    value_open = opened(value_halves, outer_turns)

    def toward(parts):
        ahead, behind = parts
        return turned(ahead, DP[0], 1), turned(behind, DP[0], -1)

    proj_around = toward(relayed(*proj_open[1:]))
    value_relay, table = lax.optimization_barrier((relayed(*value_open[1:]), table))
    value_around = toward(value_relay)
    proj_parts = sent_around(divided((proj_open[0], *proj_around), inner_turns))
    value_around, proj_parts = lax.optimization_barrier((value_around, proj_parts))
    value_parts = sent_around(divided((value_open[0], *value_around), inner_turns))
    proj_part = summed(*proj_parts)
    value_part = summed(*value_parts)
    table_part = summed_on_arrival(table, DP, 1)
    return (value_part[None], proj_part[None], table_part[None])


def solution(mesh):
    finer = Mesh(
        mesh.devices.reshape(mesh.shape["section"], 4, 4, 2), ("section", "dp_0", "dp_1", "dp_2")
    )
    placed = (
        P(None, DP, None),
        P(None, DP, None),
        P(),
        P(),
        P(),
        P("section", None, None),
        P("section", None, None),
        P("section", None, None),
    )
    return jax.shard_map(
        per_device,
        mesh=finer,
        in_specs=placed,
        out_specs=(P("section", DP, None), P("section", DP, None), P("section", None, DP)),
        check_vma=False,
    )
```

```python
import functools
import math

import jax
import jax.numpy as jnp
from jax import lax
from jax.experimental import pallas as pl
from jax.experimental.pallas import tpu as pltpu
from jax.sharding import Mesh
from jax.sharding import PartitionSpec as P

DP = ("dp_0", "dp_1", "dp_2")

NORM_FLOOR = 0.1
PARTS = 2
CHUNK = 512
PCHUNK = 512
BLOCK = 384
TALL = 768
JOINS = 2
BCHUNK = 256
GROUP = 64


def conditions(guide_bin, time_step, guide_table):
    total = guide_table.shape[1]
    half = total // 2
    frequency = jnp.exp(-math.log(10000.0) * jnp.arange(half, dtype=jnp.float32) / half)
    angle = time_step.astype(jnp.float32)[..., None] * frequency
    waves = jnp.concatenate([jnp.sin(angle), jnp.cos(angle)], axis=-1)
    bin_count = guide_table.shape[0]
    onehot = (guide_bin[..., None] == jnp.arange(bin_count, dtype=jnp.int32)).astype(jnp.float32)
    picked = jnp.einsum(
        "msb,bw->msw", onehot, guide_table.astype(jnp.float32), precision=lax.Precision.HIGHEST
    )
    return picked + 0.5 * waves


def row_mean(value):
    return jnp.sum(value, axis=-1, keepdims=True) * (1.0 / value.shape[-1])


def normalize(hidden):
    centre = row_mean(hidden)
    centred = hidden - centre
    inverse = lax.rsqrt(row_mean(centred * centred) + NORM_FLOOR)
    return (centred * inverse, inverse)


def chosen_input(place, unit, at, edge, direct, far, first_at, far_at):
    value = edge[unit, at, :]
    if direct is not None:
        value = jnp.where(place == first_at, value, direct[at, :])
    return value if far is None else jnp.where(place == far_at, far[at, :], value)


def row_groups(rows, body):
    def step(index, carry):
        body(pl.ds(pl.multiple_of(index * GROUP, GROUP), GROUP))
        return carry

    lax.fori_loop(0, rows // GROUP, step, 0)


def column_chunks(columns, body):
    def step(index, carry):
        body(pl.ds(pl.multiple_of(index * CHUNK, CHUNK), CHUNK))
        return carry

    lax.fori_loop(0, columns // CHUNK, step, 0)


def forward_kernel(tick, units, has_direct, has_far, far_at, joined, *refs):
    info, edge = refs[0], refs[1]
    rest = list(refs[2:])
    direct = rest.pop(0) if has_direct else None
    far = rest.pop(0) if has_far else None
    mod, weight = rest[0], rest[1]
    if joined:
        block_out, keep_in, keep_mod, keep_proj = rest[-4:]
    else:
        proj_weight = rest[2]
        block_out, keep_in, keep_mod, keep_proj, values = rest[-5:]
    unit = tick - info[1]
    batch = lax.div(unit, PARTS)

    @pl.when((unit >= 0) & (unit < units))
    def _():
        def modulate(at):
            block_in = chosen_input(info[0], unit, at, edge, direct, far, 0, far_at)
            keep_in[unit, at, :] = block_in
            normed, _ = normalize(block_in.astype(jnp.float32))
            shift, scale = mod[batch, 0:1, :], mod[batch, 1:2, :]
            keep_mod[unit, at, :] = (normed * (1.0 + scale) + shift).astype(jnp.bfloat16)

        row_groups(block_out.shape[0], modulate)

        def first(at):
            values[:, at] = jnp.dot(
                keep_mod[unit], weight[:, at], preferred_element_type=jnp.float32
            ).astype(jnp.bfloat16)

        if not joined:
            column_chunks(weight.shape[1], first)

        def second(at):
            if joined:
                left, right = keep_mod[unit], weight[:, at]
            else:
                left, right = values[...], proj_weight[:, at]
            projected = jnp.dot(left, right, preferred_element_type=jnp.float32)
            keep_proj[unit, :, at] = projected
            hidden = keep_in[unit, :, at].astype(jnp.float32)
            block_out[:, at] = (hidden + mod[batch, 2:3, at] * projected).astype(jnp.bfloat16)

        column_chunks(block_out.shape[1], second)


def join_kernel(part, value_weight, proj_weight, *refs):
    joined = refs[-1]
    chunks = joined.shape[1] // PCHUNK
    start = part * (joined.shape[0] // JOINS)

    def block(step, carry):
        down = pl.ds(pl.multiple_of(start + lax.div(step, chunks) * BLOCK, BLOCK), BLOCK)
        at = pl.ds(pl.multiple_of(lax.rem(step, chunks) * PCHUNK, PCHUNK), PCHUNK)
        joined[down, at] = jnp.dot(
            value_weight[down, :], proj_weight[:, at], preferred_element_type=jnp.float32
        ).astype(jnp.bfloat16)
        return carry

    lax.fori_loop(0, joined.shape[0] // JOINS // BLOCK * chunks, block, 0)


def batch_kernel(transposed, upright, left, weight, out):
    units, rows, depth = left.shape

    def chunk(at):
        flat = left[...].reshape(units * rows, depth)
        if transposed:
            total = lax.dot_general(
                flat, weight[at, :], (((1,), (1,)), ((), ())), preferred_element_type=jnp.float32
            )
        else:
            total = jnp.dot(flat, weight[:, at], preferred_element_type=jnp.float32)
        total = total.astype(jnp.bfloat16)
        if upright:
            out[at, :] = jnp.transpose(total)
        else:
            out[:, :, at] = total.reshape(units, rows, total.shape[1])

    def step(index, carry):
        chunk(pl.ds(pl.multiple_of(index * BCHUNK, BCHUNK), BCHUNK))
        return carry

    lax.fori_loop(0, weight.shape[0] // BCHUNK, step, 0)


def gate_kernel(tick, units, has_direct, has_far, first_at, far_at, *refs):
    info, edge = refs[0], refs[1]
    rest = list(refs[2:])
    direct = rest.pop(0) if has_direct else None
    far = rest.pop(0) if has_far else None
    mod, keep_gproj = rest[0], rest[-1]
    unit = tick - info[2]

    @pl.when((unit >= 0) & (unit < units))
    def _():
        def gated(at):
            upstream = chosen_input(info[0], unit, at, edge, direct, far, first_at, far_at)
            keep_gproj[unit, at, :] = (
                mod[lax.div(unit, PARTS), 2:3, :] * upstream.astype(jnp.float32)
            ).astype(jnp.bfloat16)

        row_groups(keep_gproj.shape[1], gated)


def value_kernel(tick, units, info, keep_gproj, proj_weight, keep_gval_in, keep_gval):
    unit = tick - info[2]

    @pl.when((unit >= 0) & (unit < units))
    def _():
        def chunk(at):
            keep_gval[unit, :, at] = lax.dot_general(
                keep_gproj[unit],
                proj_weight[at, :],
                (((1,), (1,)), ((), ())),
                preferred_element_type=jnp.float32,
            ).astype(jnp.bfloat16)

        column_chunks(proj_weight.shape[0], chunk)


def backward_kernel(
    tick, units, has_direct, has_far, first_at, far_at, has_table, final, *refs
):
    info, edge = refs[0], refs[1]
    rest = list(refs[2:])
    direct = rest.pop(0) if has_direct else None
    far = rest.pop(0) if has_far else None
    mod, joined, keep_in, keep_proj = rest[:4]
    table_in = rest[4] if has_table else None
    grad_mod, sums = rest[-2:]
    if final:
        keep_gproj, table_out = rest[5], rest[-3]
    else:
        grad_in, keep_gproj, table_out = rest[-5:-2]
    unit = tick - info[2]
    batch = lax.div(unit, PARTS)
    valid = (unit >= 0) & (unit < units)
    rows, width = grad_mod.shape

    @pl.when(jnp.logical_not(valid))
    def _():
        table_out[...] = jnp.zeros_like(table_out) if table_in is None else table_in[...]

    @pl.when(valid)
    def _():
        def upstream(at):
            return chosen_input(info[0], unit, at, edge, direct, far, first_at, far_at).astype(
                jnp.float32
            )

        def gated(at):
            keep_gproj[unit, at, :] = (mod[batch, 2:3, :] * upstream(at)).astype(jnp.bfloat16)

        if not final:
            row_groups(rows, gated)
        transposed = (((1,), (1,)), ((), ()))

        def second(at):
            grad_mod[:, at] = lax.dot_general(
                keep_gproj[unit], joined[at, :], transposed, preferred_element_type=jnp.float32
            )

        column_chunks(joined.shape[0], second)
        sums[...] = jnp.zeros_like(sums)

        def finish(at):
            normed, inverse = normalize(keep_in[unit, at, :].astype(jnp.float32))
            grad, grad_up = grad_mod[at, :], upstream(at)
            for index, term in enumerate((grad, grad * normed, grad_up * keep_proj[unit, at, :])):
                sums[index] += jnp.sum(term.reshape(GROUP // 8, 8, width), axis=0)
            if final:
                return
            grad_norm = grad * (1.0 + mod[batch, 1:2, :])
            centre_grad = row_mean(grad_norm)
            cross = row_mean(grad_norm * normed)
            grad_in[at, :] = (
                grad_up + inverse * (grad_norm - centre_grad - normed * cross)
            ).astype(jnp.bfloat16)

        row_groups(rows, finish)
        for index in range(3):
            total = jnp.sum(sums[index], axis=0, keepdims=True)
            table_out[index : index + 1, :] = (
                total if table_in is None else table_in[index : index + 1, :] + total
            )


def product_kernel(core, tall, right, upper, lower, staying):
    depth = tall.shape[1]
    rows = upper.shape[1]
    pairs = TALL // (2 * rows)
    chunks = right.shape[2] // PCHUNK

    def block(step, leaving, down):
        at = pl.ds(pl.multiple_of(step * PCHUNK, PCHUNK), PCHUNK)
        total = jnp.dot(
            tall[pl.ds(down * TALL, TALL), :],
            right[:, :, at].reshape(depth, PCHUNK),
            preferred_element_type=jnp.float32,
        ).astype(jnp.bfloat16)
        for pair in range(pairs):
            even = total[(2 * pair) * rows : (2 * pair + 1) * rows]
            odd = total[(2 * pair + 1) * rows : (2 * pair + 2) * rows]
            group = down * pairs + pair
            staying[group, :, at] = jnp.where(core[0] == 0, even, odd)
            leaving[pair, :, at] = jnp.where(core[0] == 0, odd, even)

    for down, leaving in enumerate((upper, lower)):

        def step(index, carry, leaving=leaving, down=down):
            block(index, leaving, down)
            return carry

        lax.fori_loop(0, chunks, step, 0)


def turn_kernel(left, tall):
    depth = left.shape[0] * left.shape[1]

    def chunk(at):
        tall[at, :] = jnp.transpose(left[:, :, at].reshape(depth, CHUNK))

    column_chunks(left.shape[2], chunk)


def open_kernel(turns, staying, upper, lower, own, ahead, behind, top, bottom):
    inner = own.shape[0]
    half = inner // 2

    def added(turn, index):
        at = turns[turn] * inner + index
        count = upper.shape[0]
        near = lax.rem(at, count)
        arrived = jnp.where(at < count, upper[near], lower[near])
        return (staying[at].astype(jnp.float32) + arrived.astype(jnp.float32)).astype(jnp.bfloat16)

    def step(index, carry):
        own[index] = added(0, index)
        ahead[index] = added(1, index)
        behind[index] = added(3, index)
        return carry

    lax.fori_loop(0, inner, step, 0)

    def halves(index, carry):
        top[index] = added(2, index)
        bottom[index] = added(2, index + half)
        return carry

    lax.fori_loop(0, half, halves, 0)


def relay_kernel(ahead, behind, above, below, ahead_out, behind_out):
    half = above.shape[0]

    def step(index, carry):
        ahead_out[index] = (
            ahead[index].astype(jnp.float32) + above[index].astype(jnp.float32)
        ).astype(jnp.bfloat16)
        behind_out[index + half] = (
            behind[index + half].astype(jnp.float32) + below[index].astype(jnp.float32)
        ).astype(jnp.bfloat16)
        return carry

    lax.fori_loop(0, half, step, 0)


def split_kernel(turns, own, first, second, *outs):
    for turn, out in enumerate(outs):
        at = turns[turn]
        out[...] = (
            own[at].astype(jnp.float32)
            + first[at].astype(jnp.float32)
            + second[at].astype(jnp.float32)
        ).astype(jnp.bfloat16)


def in_vmem(kernel, name, out_shape, operands, scalars=0, aliases=None, flops=1 << 24):
    smem, vmem = (pl.BlockSpec(memory_space=space) for space in (pltpu.SMEM, pltpu.VMEM))
    return pl.pallas_call(
        kernel,
        in_specs=[smem] * scalars + [vmem] * (len(operands) - scalars),
        out_specs=[vmem] * len(out_shape),
        out_shape=out_shape,
        input_output_aliases=aliases or {},
        cost_estimate=pl.CostEstimate(flops=flops, bytes_accessed=1 << 20, transcendentals=0),
        compiler_params=pltpu.CompilerParams(vmem_limit_bytes=10 * 1024 * 1024),
        name=name,
    )(*operands)


def bf16_of(*dims):
    return jax.ShapeDtypeStruct(dims, jnp.bfloat16)


def split_product(tall, right, core):
    outer, inner, cores = (lax.axis_size(axis) for axis in DP)
    width = right.shape[2]
    whole = bf16_of(outer * inner, tall.shape[0] // (outer * inner * cores), width)
    flops = 2 * tall.shape[0] * tall.shape[1] * width
    half = bf16_of(outer * inner // 2, *whole.shape[1:])
    return in_vmem(product_kernel, "product", [half, half, whole], (core, tall, right), 1, flops=flops)


def summed(*parts):
    total = parts[0].astype(jnp.float32)
    for part in parts[1:]:
        total = total + part.astype(jnp.float32)
    return total


def turned(value, axis, step):
    peers = lax.axis_size(axis)
    return lax.ppermute(value, axis, [(i, (i + step) % peers) for i in range(peers)])


def opened(halves, turns):
    *leaving, staying = halves
    inner = lax.axis_size(DP[1])
    rows, width = staying.shape[1:]
    arrived = [lax.ppermute(part, DP[2], [(0, 1), (1, 0)]) for part in leaving]
    full, half = bf16_of(inner, rows, width), bf16_of(inner // 2, rows, width)
    return in_vmem(
        open_kernel, "open", [full, full, full, half, half], (turns, staying, *arrived), 1
    )


def relayed(ahead, behind, top, bottom):
    above, below = turned(top, DP[0], 1), turned(bottom, DP[0], -1)
    shape = bf16_of(*ahead.shape)
    return in_vmem(
        relay_kernel, "relay", [shape] * 2, (ahead, behind, above, below), aliases={0: 0, 1: 1}
    )


def divided(parts, turns):
    shape = bf16_of(*parts[0].shape[1:])
    return in_vmem(split_kernel, "divide", [shape] * parts[0].shape[0], (turns, *parts), 1)


def sent_around(parts):
    return [parts[0]] + [turned(part, DP[1], step) for step, part in enumerate(parts[1:], 1)]


def summed_on_arrival(value, axis, dim):
    peers = lax.axis_size(axis)
    dims = value.shape
    parts = value.reshape(*dims[:dim], peers, dims[dim] // peers, *dims[dim + 1 :])
    parts = jnp.moveaxis(parts, dim, 0)
    arrived = lax.all_to_all(parts, axis, split_axis=0, concat_axis=0, tiled=True)
    return arrived.sum(axis=0)


def per_device(
    inputs, out_grad, guide_bin, time_step, guide_table, section_table, value_weight, proj_weight
):
    sections = lax.axis_size("section")
    place = lax.axis_index("section")
    batches, tok_dev, width = inputs.shape
    value_width = value_weight.shape[2]
    rows = tok_dev // PARTS
    units = batches * PARTS
    far = sections // 2
    delay = [s + (s >= far) for s in range(sections)]
    back_delay = [delay[sections - 1 - s] for s in range(sections)]
    depth = delay[-1]

    condition = conditions(guide_bin, time_step, guide_table)[:, 0]
    modulation = (condition + section_table[0].reshape(-1)).reshape(batches, 3, width)
    value_weight = value_weight[0]
    proj_weight = proj_weight[0]
    edge_in = inputs.reshape(units, rows, width)
    edge_grad = out_grad.reshape(units, rows, width)
    late = (place >= far).astype(jnp.int32)
    info = jnp.stack([place, place + late, sections - 1 - place + 1 - late]).astype(jnp.int32)
    core = lax.axis_index(DP[2]).astype(jnp.int32).reshape(1)
    turns = [
        [(lax.axis_index(axis) + step) % lax.axis_size(axis) for step in range(lax.axis_size(axis))]
        for axis in DP[:2]
    ]
    turns = [jnp.stack(turn).astype(jnp.int32) for turn in turns]
    info, core, (outer_turns, inner_turns) = lax.optimization_barrier((info, core, turns))

    vmem = pl.BlockSpec(memory_space=pltpu.VMEM)
    smem = pl.BlockSpec(memory_space=pltpu.SMEM)
    value_weight, proj_weight, edge_in, edge_grad = (
        pltpu.with_memory_space_constraint(value, pltpu.VMEM)
        for value in (value_weight, proj_weight, edge_in, edge_grad)
    )

    def slots_of(dtype):
        return jax.ShapeDtypeStruct((units, rows, width), dtype)

    flops = 2 * rows * width * value_width
    cost = pl.CostEstimate(flops=flops, bytes_accessed=16 * rows * width, transcendentals=0)
    params = pltpu.CompilerParams(vmem_limit_bytes=10 * 1024 * 1024)
    hop = jax.ShapeDtypeStruct((rows, width), jnp.bfloat16)

    def forward(tick, direct, distant, kept, weights):
        extra = [value for value in (direct, distant) if value is not None]
        operands = (info, edge_in, *extra, modulation, *weights, *kept)
        lead = len(operands) - len(kept)
        joined = len(weights) == 1
        return pl.pallas_call(
            functools.partial(
                forward_kernel, tick, units, direct is not None, distant is not None, far, joined
            ),
            in_specs=[smem] + [vmem] * (len(operands) - 1),
            out_specs=[vmem] * 4,
            out_shape=[hop]
            + [slots_of(dtype) for dtype in (jnp.bfloat16, jnp.bfloat16, jnp.float32)],
            input_output_aliases={lead + i: 1 + i for i in range(len(kept))},
            scratch_shapes=[] if joined else [pltpu.VMEM((rows, value_width), jnp.bfloat16)],
            cost_estimate=cost,
            compiler_params=params,
            name="fwd",
        )(*operands)

    def join(part, sofar):
        return pl.pallas_call(
            functools.partial(join_kernel, part),
            in_specs=[vmem] * (2 + len(sofar)),
            out_specs=vmem,
            out_shape=jax.ShapeDtypeStruct((width, width), jnp.bfloat16),
            input_output_aliases={2: 0} if sofar else {},
            cost_estimate=pl.CostEstimate(
                flops=2 * width * width * value_width // JOINS,
                bytes_accessed=6 * width * width,
                transcendentals=0,
            ),
            compiler_params=params,
            name="join",
        )(value_weight, proj_weight, *sofar)

    def batch_product(left, weight, transposed, upright):
        return pl.pallas_call(
            functools.partial(batch_kernel, transposed, upright),
            in_specs=[vmem] * 2,
            out_specs=vmem,
            out_shape=bf16_of(value_width, units * rows) if upright else slots_of(jnp.bfloat16),
            cost_estimate=pl.CostEstimate(
                flops=2 * units * rows * width * value_width,
                bytes_accessed=2 * width * width,
                transcendentals=0,
            ),
            compiler_params=params,
            name="batch",
        )(left, weight)

    def backward(tick, direct, distant, keep_in, keep_proj, sofar, final=False):
        extra = [value for value in (direct, distant) if value is not None]
        operands = (info, edge_grad, *extra, modulation, joined, keep_in, keep_proj, *sofar)
        lead = 2 + len(extra) + 4
        table_shape = jax.ShapeDtypeStruct((3, width), jnp.float32)
        if final:
            out_shape = [table_shape]
            aliases = {lead: 0}
        else:
            out_shape = [hop, slots_of(jnp.bfloat16), table_shape]
            aliases = {lead: 2, lead + 1: 1} if sofar else {}
        return pl.pallas_call(
            functools.partial(
                backward_kernel,
                tick,
                units,
                direct is not None,
                distant is not None,
                sections - 1,
                far - 1,
                bool(sofar),
                final,
            ),
            in_specs=[smem] + [vmem] * (len(operands) - 1),
            out_specs=[vmem] * len(out_shape),
            out_shape=out_shape,
            input_output_aliases=aliases,
            scratch_shapes=[
                pltpu.VMEM((rows, width), jnp.float32),
                pltpu.VMEM((3, 8, width), jnp.float32),
            ],
            cost_estimate=cost,
            compiler_params=params,
            name="bwd",
        )(*operands)

    def gate(tick, direct, distant, keep_gproj):
        extra = [value for value in (direct, distant) if value is not None]
        operands = (info, edge_grad, *extra, modulation, keep_gproj)
        return pl.pallas_call(
            functools.partial(
                gate_kernel,
                tick,
                units,
                direct is not None,
                distant is not None,
                sections - 1,
                far - 1,
            ),
            in_specs=[smem] + [vmem] * (len(operands) - 1),
            out_specs=vmem,
            out_shape=slots_of(jnp.bfloat16),
            input_output_aliases={len(operands) - 1: 0},
            cost_estimate=pl.CostEstimate(
                flops=rows * width, bytes_accessed=4 * rows * width, transcendentals=0
            ),
            compiler_params=params,
            name="gate",
        )(*operands)

    def send(value, tick, delays, step, is_far):
        pairs, wanted = [], False
        for s in range(sections):
            to = s + step
            if 0 <= to < sections and ((s < far) != (to < far)) == is_far:
                pairs.append((s, to))
                wanted = wanted or 0 <= tick - delays[s] < units
        return lax.ppermute(value, "section", pairs) if wanted else None

    kept, sofar, join_parts = [], [], []
    near_f, far_f, near_b, far_b = {}, {}, {}, {}
    last = depth + units - 1
    for tick in range(depth + last):
        if tick <= last:
            weights = [value_weight, proj_weight] if tick < JOINS else [joined]
            block_out, *kept = forward(tick, near_f.get(tick), far_f.get(tick), kept, weights)
            if tick < JOINS:
                block_out, value_weight, join_parts = lax.optimization_barrier(
                    (block_out, value_weight, join_parts)
                )
                joined = join(tick, join_parts)
                join_parts = [joined]
            near_f[tick + 1] = send(block_out, tick, delay, 1, False)
            far_f[tick + 2] = send(block_out, tick, delay, 1, True)
        back = tick - depth
        if back >= 0:
            grad_in, *rest = backward(
                back, near_b.get(back), far_b.get(back), kept[0], kept[2], sofar
            )
            sofar = [rest[1], rest[0]]
            if back == last - 4:
                grad_in, keep_mod = lax.optimization_barrier((grad_in, kept[1]))
                tall_val = batch_product(keep_mod, value_weight, False, True)
            if back == last - 5:
                grad_in, keep_mod = lax.optimization_barrier((grad_in, kept[1]))
                tall_mod = in_vmem(
                    turn_kernel, "turn", [bf16_of(width, units * rows)], (keep_mod,), flops=1 << 30
                )[0]
            if back == last - 1:
                grad_in, sofar = lax.optimization_barrier((grad_in, sofar))
                keep_gval = batch_product(sofar[1], proj_weight, True, False)
            near_b[back + 1] = send(grad_in, back, back_delay, -1, False)
            far_b[back + 2] = send(grad_in, back, back_delay, -1, True)

    direct, distant = near_b.get(last), far_b.get(last)
    table, keep_gproj = sofar
    direct, keep_gproj, keep_gval = lax.optimization_barrier((direct, keep_gproj, keep_gval))
    keep_gproj = gate(last, direct, distant, keep_gproj)
    proj_halves = split_product(tall_val, keep_gproj, core)
    right, proj_halves = lax.optimization_barrier((keep_gproj, proj_halves))
    keep_gval = in_vmem(
        functools.partial(value_kernel, last, units),
        "value",
        [slots_of(jnp.bfloat16)],
        (info, right, proj_weight, keep_gval),
        1,
        aliases={3: 0},
        flops=flops,
    )[0]
    value_halves = split_product(tall_mod, keep_gval, core)
    proj_open = opened(proj_halves, outer_turns)
    direct, proj_open = lax.optimization_barrier((direct, proj_open))
    table = backward(
        last, direct, distant, kept[0], kept[2], [table, keep_gproj], final=True
    )[0]
    value_open = opened(value_halves, outer_turns)

    def toward(parts):
        ahead, behind = parts
        return turned(ahead, DP[0], 1), turned(behind, DP[0], -1)

    proj_around = toward(relayed(*proj_open[1:]))
    value_around = toward(relayed(*value_open[1:]))
    proj_parts = sent_around(divided((proj_open[0], *proj_around), inner_turns))
    value_around, proj_parts = lax.optimization_barrier((value_around, proj_parts))
    value_divided, table = lax.optimization_barrier(
        (divided((value_open[0], *value_around), inner_turns), table)
    )
    value_parts = sent_around(value_divided)
    table_part = summed_on_arrival(table, DP, 1)
    proj_part = summed(*proj_parts)
    value_part = summed(*value_parts)
    return (value_part[None], proj_part[None], table_part[None])


def solution(mesh):
    finer = Mesh(
        mesh.devices.reshape(mesh.shape["section"], 4, 4, 2), ("section", "dp_0", "dp_1", "dp_2")
    )
    placed = (
        P(None, DP, None),
        P(None, DP, None),
        P(),
        P(),
        P(),
        P("section", None, None),
        P("section", None, None),
        P("section", None, None),
    )
    return jax.shard_map(
        per_device,
        mesh=finer,
        in_specs=placed,
        out_specs=(P("section", DP, None), P("section", DP, None), P("section", None, DP)),
        check_vma=False,
    )
```

```python
import functools
import math

import jax
import jax.numpy as jnp
from jax import lax
from jax.experimental import pallas as pl
from jax.experimental.pallas import tpu as pltpu
from jax.sharding import Mesh
from jax.sharding import PartitionSpec as P

DP = ("dp_0", "dp_1", "dp_2")

NORM_FLOOR = 0.1
PARTS = 2
CHUNK = 512
PCHUNK = 256
BLOCK = 384
JOINS = 2
BCHUNK = 128
GROUP = 64
FINISH = 32


def conditions(guide_bin, time_step, guide_table):
    total = guide_table.shape[1]
    half = total // 2
    frequency = jnp.exp(-math.log(10000.0) * jnp.arange(half, dtype=jnp.float32) / half)
    angle = time_step.astype(jnp.float32)[..., None] * frequency
    waves = jnp.concatenate([jnp.sin(angle), jnp.cos(angle)], axis=-1)
    bin_count = guide_table.shape[0]
    onehot = (guide_bin[..., None] == jnp.arange(bin_count, dtype=jnp.int32)).astype(jnp.float32)
    picked = jnp.einsum(
        "msb,bw->msw", onehot, guide_table.astype(jnp.float32), precision=lax.Precision.HIGHEST
    )
    return picked + 0.5 * waves


def row_mean(value):
    return jnp.sum(value, axis=-1, keepdims=True) * (1.0 / value.shape[-1])


def normalize(hidden):
    centre = row_mean(hidden)
    centred = hidden - centre
    inverse = lax.rsqrt(row_mean(centred * centred) + NORM_FLOOR)
    return (centred * inverse, inverse)


def chosen_input(place, unit, at, edge, direct, far, first_at, far_at):
    value = edge[unit, at, :]
    if direct is not None:
        value = jnp.where(place == first_at, value, direct[at, :])
    return value if far is None else jnp.where(place == far_at, far[at, :], value)


def row_groups(rows, body, group=GROUP):
    def step(index, carry):
        body(pl.ds(pl.multiple_of(index * group, group), group))
        return carry

    lax.fori_loop(0, rows // group, step, 0)


def column_chunks(columns, body):
    def step(index, carry):
        body(pl.ds(pl.multiple_of(index * CHUNK, CHUNK), CHUNK))
        return carry

    lax.fori_loop(0, columns // CHUNK, step, 0)


def forward_kernel(tick, units, has_direct, has_far, far_at, joined, *refs):
    info, edge = refs[0], refs[1]
    rest = list(refs[2:])
    direct = rest.pop(0) if has_direct else None
    far = rest.pop(0) if has_far else None
    mod, weight = rest[0], rest[1]
    if joined:
        block_out, keep_in, keep_mod, keep_proj = rest[-4:]
    else:
        proj_weight = rest[2]
        block_out, keep_in, keep_mod, keep_proj, values = rest[-5:]
    unit = tick - info[1]
    batch = lax.div(unit, PARTS)

    @pl.when((unit >= 0) & (unit < units))
    def _():
        def modulate(at):
            block_in = chosen_input(info[0], unit, at, edge, direct, far, 0, far_at)
            keep_in[unit, at, :] = block_in
            normed, _ = normalize(block_in.astype(jnp.float32))
            shift, scale = mod[batch, 0:1, :], mod[batch, 1:2, :]
            keep_mod[unit, at, :] = (normed * (1.0 + scale) + shift).astype(jnp.bfloat16)

        row_groups(block_out.shape[0], modulate)

        def first(at):
            values[:, at] = jnp.dot(
                keep_mod[unit], weight[:, at], preferred_element_type=jnp.float32
            ).astype(jnp.bfloat16)

        if not joined:
            column_chunks(weight.shape[1], first)

        def second(at):
            if joined:
                left, right = keep_mod[unit], weight[:, at]
            else:
                left, right = values[...], proj_weight[:, at]
            projected = jnp.dot(left, right, preferred_element_type=jnp.float32)
            keep_proj[unit, :, at] = projected
            hidden = keep_in[unit, :, at].astype(jnp.float32)
            block_out[:, at] = (hidden + mod[batch, 2:3, at] * projected).astype(jnp.bfloat16)

        column_chunks(block_out.shape[1], second)


def join_kernel(part, value_weight, proj_weight, *refs):
    joined = refs[-1]
    chunks = joined.shape[1] // PCHUNK
    start = part * (joined.shape[0] // JOINS)

    def block(step, carry):
        down = pl.ds(pl.multiple_of(start + lax.div(step, chunks) * BLOCK, BLOCK), BLOCK)
        at = pl.ds(pl.multiple_of(lax.rem(step, chunks) * PCHUNK, PCHUNK), PCHUNK)
        joined[down, at] = jnp.dot(
            value_weight[down, :], proj_weight[:, at], preferred_element_type=jnp.float32
        ).astype(jnp.bfloat16)
        return carry

    lax.fori_loop(0, joined.shape[0] // JOINS // BLOCK * chunks, block, 0)


def batch_kernel(transposed, upright, left, weight, out):
    units, rows, depth = left.shape

    def chunk(at):
        flat = left[...].reshape(units * rows, depth)
        if transposed:
            total = lax.dot_general(
                flat, weight[at, :], (((1,), (1,)), ((), ())), preferred_element_type=jnp.float32
            )
        else:
            total = jnp.dot(flat, weight[:, at], preferred_element_type=jnp.float32)
        total = total.astype(jnp.bfloat16)
        if upright:
            out[at, :] = jnp.transpose(total)
        else:
            out[:, :, at] = total.reshape(units, rows, total.shape[1])

    def step(index, carry):
        chunk(pl.ds(pl.multiple_of(index * BCHUNK, BCHUNK), BCHUNK))
        return carry

    lax.fori_loop(0, weight.shape[0] // BCHUNK, step, 0)


def gate_kernel(tick, units, has_direct, has_far, first_at, far_at, *refs):
    info, edge = refs[0], refs[1]
    rest = list(refs[2:])
    direct = rest.pop(0) if has_direct else None
    far = rest.pop(0) if has_far else None
    mod, keep_gproj = rest[0], rest[-1]
    unit = tick - info[2]

    @pl.when((unit >= 0) & (unit < units))
    def _():
        def gated(at):
            upstream = chosen_input(info[0], unit, at, edge, direct, far, first_at, far_at)
            keep_gproj[unit, at, :] = (
                mod[lax.div(unit, PARTS), 2:3, :] * upstream.astype(jnp.float32)
            ).astype(jnp.bfloat16)

        row_groups(keep_gproj.shape[1], gated)


def value_kernel(tick, units, info, keep_gproj, proj_weight, keep_gval_in, keep_gval):
    unit = tick - info[2]

    @pl.when((unit >= 0) & (unit < units))
    def _():
        def chunk(at):
            keep_gval[unit, :, at] = lax.dot_general(
                keep_gproj[unit],
                proj_weight[at, :],
                (((1,), (1,)), ((), ())),
                preferred_element_type=jnp.float32,
            ).astype(jnp.bfloat16)

        column_chunks(proj_weight.shape[0], chunk)


def backward_kernel(
    tick, units, has_direct, has_far, first_at, far_at, has_table, final, *refs
):
    info, edge = refs[0], refs[1]
    rest = list(refs[2:])
    direct = rest.pop(0) if has_direct else None
    far = rest.pop(0) if has_far else None
    mod, joined, keep_in, keep_proj = rest[:4]
    table_in = rest[4] if has_table else None
    grad_mod = rest[-1]
    if final:
        keep_gproj, table_out = rest[5], rest[-2]
    else:
        grad_in, keep_gproj, table_out = rest[-4:-1]
    unit = tick - info[2]
    batch = lax.div(unit, PARTS)
    valid = (unit >= 0) & (unit < units)
    rows, width = grad_mod.shape

    if table_in is None:
        table_out[...] = jnp.zeros_like(table_out)

    @pl.when(valid)
    def _():
        def upstream(at):
            return chosen_input(info[0], unit, at, edge, direct, far, first_at, far_at).astype(
                jnp.float32
            )

        def gated(at):
            keep_gproj[unit, at, :] = (mod[batch, 2:3, :] * upstream(at)).astype(jnp.bfloat16)

        if not final:
            row_groups(rows, gated)
        transposed = (((1,), (1,)), ((), ()))

        def second(at):
            grad_mod[:, at] = lax.dot_general(
                keep_gproj[unit], joined[at, :], transposed, preferred_element_type=jnp.float32
            )

        column_chunks(joined.shape[0], second)

        def finish(at):
            normed, inverse = normalize(keep_in[unit, at, :].astype(jnp.float32))
            grad, grad_up = grad_mod[at, :], upstream(at)
            for index, term in enumerate((grad, grad * normed, grad_up * keep_proj[unit, at, :])):
                table_out[index] += jnp.sum(term.reshape(FINISH // 8, 8, width), axis=0)
            if final:
                return
            grad_norm = grad * (1.0 + mod[batch, 1:2, :])
            centre_grad = row_mean(grad_norm)
            cross = row_mean(grad_norm * normed)
            grad_in[at, :] = (
                grad_up + inverse * (grad_norm - centre_grad - normed * cross)
            ).astype(jnp.bfloat16)

        row_groups(rows, finish, FINISH)


def product_kernel(core, tall, right, upper, lower, staying):
    depth = tall.shape[1]
    rows = upper.shape[1]
    pairs = staying.shape[0]
    each = upper.shape[0]

    def step(index, carry):
        at = pl.ds(pl.multiple_of(index * PCHUNK, PCHUNK), PCHUNK)
        total = jnp.dot(
            tall[...], right[:, :, at].reshape(depth, PCHUNK), preferred_element_type=jnp.float32
        ).astype(jnp.bfloat16)
        for pair in range(pairs):
            even = total[(2 * pair) * rows : (2 * pair + 1) * rows]
            odd = total[(2 * pair + 1) * rows : (2 * pair + 2) * rows]
            leaving = upper if pair < each else lower
            staying[pair, :, at] = jnp.where(core[0] == 0, even, odd)
            leaving[pair % each, :, at] = jnp.where(core[0] == 0, odd, even)
        return carry

    lax.fori_loop(0, right.shape[2] // PCHUNK, step, 0)


def turn_kernel(left, tall):
    depth = left.shape[0] * left.shape[1]

    def chunk(at):
        tall[at, :] = jnp.transpose(left[:, :, at].reshape(depth, CHUNK))

    column_chunks(left.shape[2], chunk)


def open_kernel(turns, staying, upper, lower, own, ahead, behind, top, bottom):
    inner = own.shape[0]
    half = inner // 2

    def added(turn, index):
        at = turns[turn] * inner + index
        count = upper.shape[0]
        near = lax.rem(at, count)
        arrived = jnp.where(at < count, upper[near], lower[near])
        return (staying[at].astype(jnp.float32) + arrived.astype(jnp.float32)).astype(jnp.bfloat16)

    def step(index, carry):
        own[index] = added(0, index)
        ahead[index] = added(1, index)
        behind[index] = added(3, index)
        return carry

    lax.fori_loop(0, inner, step, 0)

    def halves(index, carry):
        top[index] = added(2, index)
        bottom[index] = added(2, index + half)
        return carry

    lax.fori_loop(0, half, halves, 0)


def relay_kernel(ahead, behind, above, below, ahead_out, behind_out):
    half = above.shape[0]

    def step(index, carry):
        ahead_out[index] = (
            ahead[index].astype(jnp.float32) + above[index].astype(jnp.float32)
        ).astype(jnp.bfloat16)
        behind_out[index + half] = (
            behind[index + half].astype(jnp.float32) + below[index].astype(jnp.float32)
        ).astype(jnp.bfloat16)
        return carry

    lax.fori_loop(0, half, step, 0)


def split_kernel(turns, own, first, second, *outs):
    for turn, out in enumerate(outs):
        at = turns[turn]
        out[...] = (
            own[at].astype(jnp.float32)
            + first[at].astype(jnp.float32)
            + second[at].astype(jnp.float32)
        ).astype(jnp.bfloat16)


def in_vmem(kernel, name, out_shape, operands, scalars=0, aliases=None, flops=1 << 24):
    smem, vmem = (pl.BlockSpec(memory_space=space) for space in (pltpu.SMEM, pltpu.VMEM))
    return pl.pallas_call(
        kernel,
        in_specs=[smem] * scalars + [vmem] * (len(operands) - scalars),
        out_specs=[vmem] * len(out_shape),
        out_shape=out_shape,
        input_output_aliases=aliases or {},
        cost_estimate=pl.CostEstimate(flops=flops, bytes_accessed=1 << 20, transcendentals=0),
        compiler_params=pltpu.CompilerParams(vmem_limit_bytes=10 * 1024 * 1024),
        name=name,
    )(*operands)


def bf16_of(*dims):
    return jax.ShapeDtypeStruct(dims, jnp.bfloat16)


def split_product(tall, right, core):
    outer, inner, cores = (lax.axis_size(axis) for axis in DP)
    width = right.shape[2]
    whole = bf16_of(outer * inner, tall.shape[0] // (outer * inner * cores), width)
    flops = 2 * tall.shape[0] * tall.shape[1] * width
    half = bf16_of(outer * inner // 2, *whole.shape[1:])
    return in_vmem(product_kernel, "product", [half, half, whole], (core, tall, right), 1, flops=flops)


def summed(*parts):
    total = parts[0].astype(jnp.float32)
    for part in parts[1:]:
        total = total + part.astype(jnp.float32)
    return total


def turned(value, axis, step):
    peers = lax.axis_size(axis)
    return lax.ppermute(value, axis, [(i, (i + step) % peers) for i in range(peers)])


def opened(halves, turns):
    *leaving, staying = halves
    inner = lax.axis_size(DP[1])
    rows, width = staying.shape[1:]
    arrived = [lax.ppermute(part, DP[2], [(0, 1), (1, 0)]) for part in leaving]
    full, half = bf16_of(inner, rows, width), bf16_of(inner // 2, rows, width)
    return in_vmem(
        open_kernel, "open", [full, full, full, half, half], (turns, staying, *arrived), 1
    )


def relayed(ahead, behind, top, bottom):
    above, below = turned(top, DP[0], 1), turned(bottom, DP[0], -1)
    shape = bf16_of(*ahead.shape)
    return in_vmem(
        relay_kernel, "relay", [shape] * 2, (ahead, behind, above, below), aliases={0: 0, 1: 1}
    )


def divided(parts, turns):
    shape = bf16_of(*parts[0].shape[1:])
    return in_vmem(split_kernel, "divide", [shape] * parts[0].shape[0], (turns, *parts), 1)


def sent_around(parts):
    return [parts[0]] + [turned(part, DP[1], step) for step, part in enumerate(parts[1:], 1)]


def summed_on_arrival(value, axis, dim):
    peers = lax.axis_size(axis)
    dims = value.shape
    parts = value.reshape(*dims[:dim], peers, dims[dim] // peers, *dims[dim + 1 :])
    parts = jnp.moveaxis(parts, dim, 0)
    arrived = lax.all_to_all(parts, axis, split_axis=0, concat_axis=0, tiled=True)
    return arrived.sum(axis=0)


def per_device(
    inputs, out_grad, guide_bin, time_step, guide_table, section_table, value_weight, proj_weight
):
    sections = lax.axis_size("section")
    place = lax.axis_index("section")
    batches, tok_dev, width = inputs.shape
    value_width = value_weight.shape[2]
    rows = tok_dev // PARTS
    units = batches * PARTS
    far = sections // 2
    delay = [s + (s >= far) for s in range(sections)]
    back_delay = [delay[sections - 1 - s] for s in range(sections)]
    depth = delay[-1]

    condition = conditions(guide_bin, time_step, guide_table)[:, 0]
    modulation = (condition + section_table[0].reshape(-1)).reshape(batches, 3, width)
    value_weight = value_weight[0]
    proj_weight = proj_weight[0]
    edge_in = inputs.reshape(units, rows, width)
    edge_grad = out_grad.reshape(units, rows, width)
    late = (place >= far).astype(jnp.int32)
    info = jnp.stack([place, place + late, sections - 1 - place + 1 - late]).astype(jnp.int32)
    core = lax.axis_index(DP[2]).astype(jnp.int32).reshape(1)
    turns = [
        [(lax.axis_index(axis) + step) % lax.axis_size(axis) for step in range(lax.axis_size(axis))]
        for axis in DP[:2]
    ]
    turns = [jnp.stack(turn).astype(jnp.int32) for turn in turns]
    info, core, (outer_turns, inner_turns) = lax.optimization_barrier((info, core, turns))

    vmem = pl.BlockSpec(memory_space=pltpu.VMEM)
    smem = pl.BlockSpec(memory_space=pltpu.SMEM)
    value_weight, proj_weight, edge_in, edge_grad = (
        pltpu.with_memory_space_constraint(value, pltpu.VMEM)
        for value in (value_weight, proj_weight, edge_in, edge_grad)
    )

    def slots_of(dtype):
        return jax.ShapeDtypeStruct((units, rows, width), dtype)

    flops = 2 * rows * width * value_width
    cost = pl.CostEstimate(flops=flops, bytes_accessed=16 * rows * width, transcendentals=0)
    params = pltpu.CompilerParams(vmem_limit_bytes=10 * 1024 * 1024)
    hop = jax.ShapeDtypeStruct((rows, width), jnp.bfloat16)

    def forward(tick, direct, distant, kept, weights):
        extra = [value for value in (direct, distant) if value is not None]
        operands = (info, edge_in, *extra, modulation, *weights, *kept)
        lead = len(operands) - len(kept)
        joined = len(weights) == 1
        return pl.pallas_call(
            functools.partial(
                forward_kernel, tick, units, direct is not None, distant is not None, far, joined
            ),
            in_specs=[smem] + [vmem] * (len(operands) - 1),
            out_specs=[vmem] * 4,
            out_shape=[hop]
            + [slots_of(dtype) for dtype in (jnp.bfloat16, jnp.bfloat16, jnp.float32)],
            input_output_aliases={lead + i: 1 + i for i in range(len(kept))},
            scratch_shapes=[] if joined else [pltpu.VMEM((rows, value_width), jnp.bfloat16)],
            cost_estimate=cost,
            compiler_params=params,
            name="fwd",
        )(*operands)

    def join(part, sofar):
        return pl.pallas_call(
            functools.partial(join_kernel, part),
            in_specs=[vmem] * (2 + len(sofar)),
            out_specs=vmem,
            out_shape=jax.ShapeDtypeStruct((width, width), jnp.bfloat16),
            input_output_aliases={2: 0} if sofar else {},
            cost_estimate=pl.CostEstimate(
                flops=2 * width * width * value_width // JOINS,
                bytes_accessed=6 * width * width,
                transcendentals=0,
            ),
            compiler_params=params,
            name="join",
        )(value_weight, proj_weight, *sofar)

    def batch_product(left, weight, transposed, upright):
        return pl.pallas_call(
            functools.partial(batch_kernel, transposed, upright),
            in_specs=[vmem] * 2,
            out_specs=vmem,
            out_shape=bf16_of(value_width, units * rows) if upright else slots_of(jnp.bfloat16),
            cost_estimate=pl.CostEstimate(
                flops=2 * units * rows * width * value_width,
                bytes_accessed=2 * width * width,
                transcendentals=0,
            ),
            compiler_params=params,
            name="batch",
        )(left, weight)

    def backward(tick, direct, distant, keep_in, keep_proj, sofar, final=False):
        extra = [value for value in (direct, distant) if value is not None]
        operands = (info, edge_grad, *extra, modulation, joined, keep_in, keep_proj, *sofar)
        lead = 2 + len(extra) + 4
        table_shape = jax.ShapeDtypeStruct((3, 8, width), jnp.float32)
        if final:
            out_shape = [table_shape]
            aliases = {lead: 0}
        else:
            out_shape = [hop, slots_of(jnp.bfloat16), table_shape]
            aliases = {lead: 2, lead + 1: 1} if sofar else {}
        return pl.pallas_call(
            functools.partial(
                backward_kernel,
                tick,
                units,
                direct is not None,
                distant is not None,
                sections - 1,
                far - 1,
                bool(sofar),
                final,
            ),
            in_specs=[smem] + [vmem] * (len(operands) - 1),
            out_specs=[vmem] * len(out_shape),
            out_shape=out_shape,
            input_output_aliases=aliases,
            scratch_shapes=[
                pltpu.VMEM((rows, width), jnp.float32),
            ],
            cost_estimate=cost,
            compiler_params=params,
            name="bwd",
        )(*operands)

    def gate(tick, direct, distant, keep_gproj):
        extra = [value for value in (direct, distant) if value is not None]
        operands = (info, edge_grad, *extra, modulation, keep_gproj)
        return pl.pallas_call(
            functools.partial(
                gate_kernel,
                tick,
                units,
                direct is not None,
                distant is not None,
                sections - 1,
                far - 1,
            ),
            in_specs=[smem] + [vmem] * (len(operands) - 1),
            out_specs=vmem,
            out_shape=slots_of(jnp.bfloat16),
            input_output_aliases={len(operands) - 1: 0},
            cost_estimate=pl.CostEstimate(
                flops=rows * width, bytes_accessed=4 * rows * width, transcendentals=0
            ),
            compiler_params=params,
            name="gate",
        )(*operands)

    def send(value, tick, delays, step, is_far):
        pairs, wanted = [], False
        for s in range(sections):
            to = s + step
            if 0 <= to < sections and ((s < far) != (to < far)) == is_far:
                pairs.append((s, to))
                wanted = wanted or 0 <= tick - delays[s] < units
        return lax.ppermute(value, "section", pairs) if wanted else None

    kept, sofar, join_parts = [], [], []
    near_f, far_f, near_b, far_b = {}, {}, {}, {}
    last = depth + units - 1
    for tick in range(depth + last):
        if tick <= last:
            weights = [value_weight, proj_weight] if tick < JOINS else [joined]
            block_out, *kept = forward(tick, near_f.get(tick), far_f.get(tick), kept, weights)
            if tick < JOINS:
                block_out, value_weight, join_parts = lax.optimization_barrier(
                    (block_out, value_weight, join_parts)
                )
                joined = join(tick, join_parts)
                join_parts = [joined]
            near_f[tick + 1] = send(block_out, tick, delay, 1, False)
            far_f[tick + 2] = send(block_out, tick, delay, 1, True)
        back = tick - depth
        if back >= 0:
            grad_in, *rest = backward(
                back, near_b.get(back), far_b.get(back), kept[0], kept[2], sofar
            )
            sofar = [rest[1], rest[0]]
            if back == last - 4:
                grad_in, keep_mod = lax.optimization_barrier((grad_in, kept[1]))
                tall_val = batch_product(keep_mod, value_weight, False, True)
            if back == last - 5:
                grad_in, keep_mod = lax.optimization_barrier((grad_in, kept[1]))
                tall_mod = in_vmem(
                    turn_kernel, "turn", [bf16_of(width, units * rows)], (keep_mod,), flops=1 << 30
                )[0]
            if back == last - 1:
                grad_in, sofar = lax.optimization_barrier((grad_in, sofar))
                keep_gval = batch_product(sofar[1], proj_weight, True, False)
            near_b[back + 1] = send(grad_in, back, back_delay, -1, False)
            far_b[back + 2] = send(grad_in, back, back_delay, -1, True)

    direct, distant = near_b.get(last), far_b.get(last)
    table, keep_gproj = sofar
    direct, keep_gproj, keep_gval = lax.optimization_barrier((direct, keep_gproj, keep_gval))
    keep_gproj = gate(last, direct, distant, keep_gproj)
    proj_halves = split_product(tall_val, keep_gproj, core)
    right, proj_halves = lax.optimization_barrier((keep_gproj, proj_halves))
    keep_gval = in_vmem(
        functools.partial(value_kernel, last, units),
        "value",
        [slots_of(jnp.bfloat16)],
        (info, right, proj_weight, keep_gval),
        1,
        aliases={3: 0},
        flops=flops,
    )[0]
    value_halves = split_product(tall_mod, keep_gval, core)
    proj_open = opened(proj_halves, outer_turns)
    direct, proj_open = lax.optimization_barrier((direct, proj_open))
    table = backward(
        last, direct, distant, kept[0], kept[2], [table, keep_gproj], final=True
    )[0]
    value_open = opened(value_halves, outer_turns)

    def toward(parts):
        ahead, behind = parts
        return turned(ahead, DP[0], 1), turned(behind, DP[0], -1)

    proj_around = toward(relayed(*proj_open[1:]))
    value_around = toward(relayed(*value_open[1:]))
    proj_parts = sent_around(divided((proj_open[0], *proj_around), inner_turns))
    value_around, proj_parts = lax.optimization_barrier((value_around, proj_parts))
    value_divided, table = lax.optimization_barrier(
        (divided((value_open[0], *value_around), inner_turns), table)
    )
    value_parts = sent_around(value_divided)
    table_part = summed_on_arrival(jnp.sum(table, axis=1), DP, 1)
    proj_part = summed(*proj_parts)
    value_part = summed(*value_parts)
    return (value_part[None], proj_part[None], table_part[None])


def solution(mesh):
    finer = Mesh(
        mesh.devices.reshape(mesh.shape["section"], 4, 4, 2), ("section", "dp_0", "dp_1", "dp_2")
    )
    placed = (
        P(None, DP, None),
        P(None, DP, None),
        P(),
        P(),
        P(),
        P("section", None, None),
        P("section", None, None),
        P("section", None, None),
    )
    return jax.shard_map(
        per_device,
        mesh=finer,
        in_specs=placed,
        out_specs=(P("section", DP, None), P("section", DP, None), P("section", None, DP)),
        check_vma=False,
    )
```

```python
import functools
import math

import jax
import jax.numpy as jnp
from jax import lax
from jax.experimental import pallas as pl
from jax.experimental.pallas import tpu as pltpu
from jax.sharding import Mesh
from jax.sharding import PartitionSpec as P

DP = ("dp_0", "dp_1", "dp_2")

NORM_FLOOR = 0.1
PARTS = 2
CHUNK = 512
PCHUNK = 256
BLOCK = 384
JOINS = 2
BCHUNK = 128
GROUP = 64
FINISH = 32


def conditions(guide_bin, time_step, guide_table):
    total = guide_table.shape[1]
    half = total // 2
    frequency = jnp.exp(-math.log(10000.0) * jnp.arange(half, dtype=jnp.float32) / half)
    angle = time_step.astype(jnp.float32)[..., None] * frequency
    waves = jnp.concatenate([jnp.sin(angle), jnp.cos(angle)], axis=-1)
    bin_count = guide_table.shape[0]
    onehot = (guide_bin[..., None] == jnp.arange(bin_count, dtype=jnp.int32)).astype(jnp.float32)
    picked = jnp.einsum(
        "msb,bw->msw", onehot, guide_table.astype(jnp.float32), precision=lax.Precision.HIGHEST
    )
    return picked + 0.5 * waves


def row_mean(value):
    return jnp.sum(value, axis=-1, keepdims=True) * (1.0 / value.shape[-1])


def normalize(hidden):
    centre = row_mean(hidden)
    centred = hidden - centre
    inverse = lax.rsqrt(row_mean(centred * centred) + NORM_FLOOR)
    return (centred * inverse, inverse)


def chosen_input(place, unit, at, edge, direct, far, first_at, far_at):
    value = edge[unit, at, :]
    if direct is not None:
        value = jnp.where(place == first_at, value, direct[at, :])
    return value if far is None else jnp.where(place == far_at, far[at, :], value)


def row_groups(rows, body, group=GROUP):
    def step(index, carry):
        body(pl.ds(pl.multiple_of(index * group, group), group))
        return carry

    lax.fori_loop(0, rows // group, step, 0)


def column_chunks(columns, body):
    def step(index, carry):
        body(pl.ds(pl.multiple_of(index * CHUNK, CHUNK), CHUNK))
        return carry

    lax.fori_loop(0, columns // CHUNK, step, 0)


def forward_kernel(tick, units, has_direct, has_far, far_at, joined, *refs):
    info, edge = refs[0], refs[1]
    rest = list(refs[2:])
    direct = rest.pop(0) if has_direct else None
    far = rest.pop(0) if has_far else None
    mod, weight = rest[0], rest[1]
    if joined:
        block_out, keep_in, keep_mod, keep_proj = rest[-4:]
    else:
        proj_weight = rest[2]
        block_out, keep_in, keep_mod, keep_proj, values = rest[-5:]
    unit = tick - info[1]
    batch = lax.div(unit, PARTS)

    @pl.when((unit >= 0) & (unit < units))
    def _():
        def modulate(at):
            block_in = chosen_input(info[0], unit, at, edge, direct, far, 0, far_at)
            keep_in[unit, at, :] = block_in
            normed, _ = normalize(block_in.astype(jnp.float32))
            shift, scale = mod[batch, 0:1, :], mod[batch, 1:2, :]
            keep_mod[unit, at, :] = (normed * (1.0 + scale) + shift).astype(jnp.bfloat16)

        row_groups(block_out.shape[0], modulate)

        def first(at):
            values[:, at] = jnp.dot(
                keep_mod[unit], weight[:, at], preferred_element_type=jnp.float32
            ).astype(jnp.bfloat16)

        if not joined:
            column_chunks(weight.shape[1], first)

        def second(at):
            if joined:
                left, right = keep_mod[unit], weight[:, at]
            else:
                left, right = values[...], proj_weight[:, at]
            projected = jnp.dot(left, right, preferred_element_type=jnp.float32)
            keep_proj[unit, :, at] = projected
            hidden = keep_in[unit, :, at].astype(jnp.float32)
            block_out[:, at] = (hidden + mod[batch, 2:3, at] * projected).astype(jnp.bfloat16)

        column_chunks(block_out.shape[1], second)


def join_kernel(part, value_weight, proj_weight, *refs):
    joined = refs[-1]
    chunks = joined.shape[1] // PCHUNK
    start = part * (joined.shape[0] // JOINS)

    def block(step, carry):
        down = pl.ds(pl.multiple_of(start + lax.div(step, chunks) * BLOCK, BLOCK), BLOCK)
        at = pl.ds(pl.multiple_of(lax.rem(step, chunks) * PCHUNK, PCHUNK), PCHUNK)
        joined[down, at] = jnp.dot(
            value_weight[down, :], proj_weight[:, at], preferred_element_type=jnp.float32
        ).astype(jnp.bfloat16)
        return carry

    lax.fori_loop(0, joined.shape[0] // JOINS // BLOCK * chunks, block, 0)


def batch_kernel(transposed, upright, left, weight, out):
    units, rows, depth = left.shape

    def chunk(at):
        flat = left[...].reshape(units * rows, depth)
        if transposed:
            total = lax.dot_general(
                flat, weight[at, :], (((1,), (1,)), ((), ())), preferred_element_type=jnp.float32
            )
        else:
            total = jnp.dot(flat, weight[:, at], preferred_element_type=jnp.float32)
        total = total.astype(jnp.bfloat16)
        if upright:
            out[at, :] = jnp.transpose(total)
        else:
            out[:, :, at] = total.reshape(units, rows, total.shape[1])

    def step(index, carry):
        chunk(pl.ds(pl.multiple_of(index * BCHUNK, BCHUNK), BCHUNK))
        return carry

    lax.fori_loop(0, weight.shape[0] // BCHUNK, step, 0)


def gate_kernel(tick, units, has_direct, has_far, first_at, far_at, *refs):
    info, edge = refs[0], refs[1]
    rest = list(refs[2:])
    direct = rest.pop(0) if has_direct else None
    far = rest.pop(0) if has_far else None
    mod, keep_gproj = rest[0], rest[-1]
    unit = tick - info[2]

    @pl.when((unit >= 0) & (unit < units))
    def _():
        def gated(at):
            upstream = chosen_input(info[0], unit, at, edge, direct, far, first_at, far_at)
            keep_gproj[unit, at, :] = (
                mod[lax.div(unit, PARTS), 2:3, :] * upstream.astype(jnp.float32)
            ).astype(jnp.bfloat16)

        row_groups(keep_gproj.shape[1], gated)


def value_kernel(tick, units, info, keep_gproj, proj_weight, keep_gval_in, keep_gval):
    unit = tick - info[2]

    @pl.when((unit >= 0) & (unit < units))
    def _():
        def chunk(at):
            keep_gval[unit, :, at] = lax.dot_general(
                keep_gproj[unit],
                proj_weight[at, :],
                (((1,), (1,)), ((), ())),
                preferred_element_type=jnp.float32,
            ).astype(jnp.bfloat16)

        column_chunks(proj_weight.shape[0], chunk)


def backward_kernel(
    tick, units, has_direct, has_far, first_at, far_at, has_table, final, *refs
):
    info, edge = refs[0], refs[1]
    rest = list(refs[2:])
    direct = rest.pop(0) if has_direct else None
    far = rest.pop(0) if has_far else None
    mod, joined, keep_in, keep_proj = rest[:4]
    table_in = rest[4] if has_table else None
    grad_mod = rest[-1]
    if final:
        keep_gproj, table_out = rest[5], rest[-2]
    else:
        grad_in, keep_gproj, table_out = rest[-4:-1]
    unit = tick - info[2]
    batch = lax.div(unit, PARTS)
    valid = (unit >= 0) & (unit < units)
    rows, width = grad_mod.shape

    if table_in is None:
        table_out[...] = jnp.zeros_like(table_out)

    @pl.when(valid)
    def _():
        def upstream(at):
            return chosen_input(info[0], unit, at, edge, direct, far, first_at, far_at).astype(
                jnp.float32
            )

        def gated(at):
            keep_gproj[unit, at, :] = (mod[batch, 2:3, :] * upstream(at)).astype(jnp.bfloat16)

        if not final:
            row_groups(rows, gated)
        transposed = (((1,), (1,)), ((), ()))

        def second(at):
            grad_mod[:, at] = lax.dot_general(
                keep_gproj[unit], joined[at, :], transposed, preferred_element_type=jnp.float32
            )

        column_chunks(joined.shape[0], second)

        def finish(at):
            normed, inverse = normalize(keep_in[unit, at, :].astype(jnp.float32))
            grad, grad_up = grad_mod[at, :], upstream(at)
            for index, term in enumerate((grad, grad * normed, grad_up * keep_proj[unit, at, :])):
                table_out[index] += jnp.sum(term.reshape(FINISH // 8, 8, width), axis=0)
            if final:
                return
            grad_norm = grad * (1.0 + mod[batch, 1:2, :])
            centre_grad = row_mean(grad_norm)
            cross = row_mean(grad_norm * normed)
            grad_in[at, :] = (
                grad_up + inverse * (grad_norm - centre_grad - normed * cross)
            ).astype(jnp.bfloat16)

        row_groups(rows, finish, FINISH)


def product_kernel(core, tall, right, upper, lower, staying):
    depth = tall.shape[1]
    rows = upper.shape[1]
    pairs = staying.shape[0]
    each = upper.shape[0]

    def step(index, carry):
        at = pl.ds(pl.multiple_of(index * PCHUNK, PCHUNK), PCHUNK)
        total = jnp.dot(
            tall[...], right[:, :, at].reshape(depth, PCHUNK), preferred_element_type=jnp.float32
        ).astype(jnp.bfloat16)
        for pair in range(pairs):
            even = total[(2 * pair) * rows : (2 * pair + 1) * rows]
            odd = total[(2 * pair + 1) * rows : (2 * pair + 2) * rows]
            leaving = upper if pair < each else lower
            staying[pair, :, at] = jnp.where(core[0] == 0, even, odd)
            leaving[pair % each, :, at] = jnp.where(core[0] == 0, odd, even)
        return carry

    lax.fori_loop(0, right.shape[2] // PCHUNK, step, 0)


def turn_kernel(left, tall):
    depth = left.shape[0] * left.shape[1]

    def chunk(at):
        tall[at, :] = jnp.transpose(left[:, :, at].reshape(depth, CHUNK))

    column_chunks(left.shape[2], chunk)


def open_kernel(turns, staying, upper, lower, own, ahead, behind, top, bottom):
    inner = own.shape[0]
    half = inner // 2

    def added(turn, index):
        at = turns[turn] * inner + index
        count = upper.shape[0]
        near = lax.rem(at, count)
        arrived = jnp.where(at < count, upper[near], lower[near])
        return (staying[at].astype(jnp.float32) + arrived.astype(jnp.float32)).astype(jnp.bfloat16)

    def step(index, carry):
        own[index] = added(0, index)
        ahead[index] = added(1, index)
        behind[index] = added(3, index)
        return carry

    lax.fori_loop(0, inner, step, 0)

    def halves(index, carry):
        top[index] = added(2, index)
        bottom[index] = added(2, index + half)
        return carry

    lax.fori_loop(0, half, halves, 0)


def relay_kernel(ahead, behind, above, below, ahead_out, behind_out):
    half = above.shape[0]

    def step(index, carry):
        ahead_out[index] = (
            ahead[index].astype(jnp.float32) + above[index].astype(jnp.float32)
        ).astype(jnp.bfloat16)
        behind_out[index + half] = (
            behind[index + half].astype(jnp.float32) + below[index].astype(jnp.float32)
        ).astype(jnp.bfloat16)
        return carry

    lax.fori_loop(0, half, step, 0)


def split_kernel(turns, own, first, second, *outs):
    for turn, out in enumerate(outs):
        at = turns[turn]
        out[...] = (
            own[at].astype(jnp.float32)
            + first[at].astype(jnp.float32)
            + second[at].astype(jnp.float32)
        ).astype(jnp.bfloat16)


def in_vmem(kernel, name, out_shape, operands, scalars=0, aliases=None, flops=1 << 24):
    smem, vmem = (pl.BlockSpec(memory_space=space) for space in (pltpu.SMEM, pltpu.VMEM))
    return pl.pallas_call(
        kernel,
        in_specs=[smem] * scalars + [vmem] * (len(operands) - scalars),
        out_specs=[vmem] * len(out_shape),
        out_shape=out_shape,
        input_output_aliases=aliases or {},
        cost_estimate=pl.CostEstimate(flops=flops, bytes_accessed=1 << 20, transcendentals=0),
        compiler_params=pltpu.CompilerParams(vmem_limit_bytes=10 * 1024 * 1024),
        name=name,
    )(*operands)


def bf16_of(*dims):
    return jax.ShapeDtypeStruct(dims, jnp.bfloat16)


def split_product(tall, right, core):
    outer, inner, cores = (lax.axis_size(axis) for axis in DP)
    width = right.shape[2]
    whole = bf16_of(outer * inner, tall.shape[0] // (outer * inner * cores), width)
    flops = 2 * tall.shape[0] * tall.shape[1] * width
    half = bf16_of(outer * inner // 2, *whole.shape[1:])
    return in_vmem(product_kernel, "product", [half, half, whole], (core, tall, right), 1, flops=flops)


def summed(*parts):
    total = parts[0].astype(jnp.float32)
    for part in parts[1:]:
        total = total + part.astype(jnp.float32)
    return total


def turned(value, axis, step):
    peers = lax.axis_size(axis)
    return lax.ppermute(value, axis, [(i, (i + step) % peers) for i in range(peers)])


def opened(halves, turns):
    *leaving, staying = halves
    inner = lax.axis_size(DP[1])
    rows, width = staying.shape[1:]
    arrived = [lax.ppermute(part, DP[2], [(0, 1), (1, 0)]) for part in leaving]
    full, half = bf16_of(inner, rows, width), bf16_of(inner // 2, rows, width)
    return in_vmem(
        open_kernel, "open", [full, full, full, half, half], (turns, staying, *arrived), 1
    )


def relayed(ahead, behind, top, bottom):
    above, below = turned(top, DP[0], 1), turned(bottom, DP[0], -1)
    shape = bf16_of(*ahead.shape)
    return in_vmem(
        relay_kernel, "relay", [shape] * 2, (ahead, behind, above, below), aliases={0: 0, 1: 1}
    )


def divided(parts, turns):
    shape = bf16_of(*parts[0].shape[1:])
    return in_vmem(split_kernel, "divide", [shape] * parts[0].shape[0], (turns, *parts), 1)


def sent_around(parts):
    return [parts[0]] + [turned(part, DP[1], step) for step, part in enumerate(parts[1:], 1)]


def summed_on_arrival(value, axis, dim):
    peers = lax.axis_size(axis)
    dims = value.shape
    parts = value.reshape(*dims[:dim], peers, dims[dim] // peers, *dims[dim + 1 :])
    parts = jnp.moveaxis(parts, dim, 0)
    arrived = lax.all_to_all(parts, axis, split_axis=0, concat_axis=0, tiled=True)
    return arrived.sum(axis=0)


def per_device(
    inputs, out_grad, guide_bin, time_step, guide_table, section_table, value_weight, proj_weight
):
    sections = lax.axis_size("section")
    place = lax.axis_index("section")
    batches, tok_dev, width = inputs.shape
    value_width = value_weight.shape[2]
    rows = tok_dev // PARTS
    units = batches * PARTS
    far = sections // 2
    delay = [s + (s >= far) for s in range(sections)]
    back_delay = [delay[sections - 1 - s] for s in range(sections)]
    depth = delay[-1]

    condition = conditions(guide_bin, time_step, guide_table)[:, 0]
    modulation = (condition + section_table[0].reshape(-1)).reshape(batches, 3, width)
    value_weight = value_weight[0]
    proj_weight = proj_weight[0]
    edge_in = inputs.reshape(units, rows, width)
    edge_grad = out_grad.reshape(units, rows, width)
    late = (place >= far).astype(jnp.int32)
    info = jnp.stack([place, place + late, sections - 1 - place + 1 - late]).astype(jnp.int32)
    core = lax.axis_index(DP[2]).astype(jnp.int32).reshape(1)
    turns = [
        [(lax.axis_index(axis) + step) % lax.axis_size(axis) for step in range(lax.axis_size(axis))]
        for axis in DP[:2]
    ]
    turns = [jnp.stack(turn).astype(jnp.int32) for turn in turns]
    info, core, (outer_turns, inner_turns) = lax.optimization_barrier((info, core, turns))

    vmem = pl.BlockSpec(memory_space=pltpu.VMEM)
    smem = pl.BlockSpec(memory_space=pltpu.SMEM)
    value_weight, proj_weight, edge_in, edge_grad = (
        pltpu.with_memory_space_constraint(value, pltpu.VMEM)
        for value in (value_weight, proj_weight, edge_in, edge_grad)
    )

    def slots_of(dtype):
        return jax.ShapeDtypeStruct((units, rows, width), dtype)

    flops = 2 * rows * width * value_width
    cost = pl.CostEstimate(flops=flops, bytes_accessed=16 * rows * width, transcendentals=0)
    params = pltpu.CompilerParams(vmem_limit_bytes=10 * 1024 * 1024)
    hop = jax.ShapeDtypeStruct((rows, width), jnp.bfloat16)

    def forward(tick, direct, distant, kept, weights):
        extra = [value for value in (direct, distant) if value is not None]
        operands = (info, edge_in, *extra, modulation, *weights, *kept)
        lead = len(operands) - len(kept)
        joined = len(weights) == 1
        return pl.pallas_call(
            functools.partial(
                forward_kernel, tick, units, direct is not None, distant is not None, far, joined
            ),
            in_specs=[smem] + [vmem] * (len(operands) - 1),
            out_specs=[vmem] * 4,
            out_shape=[hop]
            + [slots_of(dtype) for dtype in (jnp.bfloat16, jnp.bfloat16, jnp.float32)],
            input_output_aliases={lead + i: 1 + i for i in range(len(kept))},
            scratch_shapes=[] if joined else [pltpu.VMEM((rows, value_width), jnp.bfloat16)],
            cost_estimate=cost,
            compiler_params=params,
            name="fwd",
        )(*operands)

    def join(part, sofar):
        return pl.pallas_call(
            functools.partial(join_kernel, part),
            in_specs=[vmem] * (2 + len(sofar)),
            out_specs=vmem,
            out_shape=jax.ShapeDtypeStruct((width, width), jnp.bfloat16),
            input_output_aliases={2: 0} if sofar else {},
            cost_estimate=pl.CostEstimate(
                flops=2 * width * width * value_width // JOINS,
                bytes_accessed=6 * width * width,
                transcendentals=0,
            ),
            compiler_params=params,
            name="join",
        )(value_weight, proj_weight, *sofar)

    def batch_product(left, weight, transposed, upright):
        return pl.pallas_call(
            functools.partial(batch_kernel, transposed, upright),
            in_specs=[vmem] * 2,
            out_specs=vmem,
            out_shape=bf16_of(value_width, units * rows) if upright else slots_of(jnp.bfloat16),
            cost_estimate=pl.CostEstimate(
                flops=2 * units * rows * width * value_width,
                bytes_accessed=2 * width * width,
                transcendentals=0,
            ),
            compiler_params=params,
            name="batch",
        )(left, weight)

    def backward(tick, direct, distant, keep_in, keep_proj, sofar, final=False):
        extra = [value for value in (direct, distant) if value is not None]
        operands = (info, edge_grad, *extra, modulation, joined, keep_in, keep_proj, *sofar)
        lead = 2 + len(extra) + 4
        table_shape = jax.ShapeDtypeStruct((3, 8, width), jnp.float32)
        if final:
            out_shape = [table_shape]
            aliases = {lead: 0}
        else:
            out_shape = [hop, slots_of(jnp.bfloat16), table_shape]
            aliases = {lead: 2, lead + 1: 1} if sofar else {}
        return pl.pallas_call(
            functools.partial(
                backward_kernel,
                tick,
                units,
                direct is not None,
                distant is not None,
                sections - 1,
                far - 1,
                bool(sofar),
                final,
            ),
            in_specs=[smem] + [vmem] * (len(operands) - 1),
            out_specs=[vmem] * len(out_shape),
            out_shape=out_shape,
            input_output_aliases=aliases,
            scratch_shapes=[
                pltpu.VMEM((rows, width), jnp.float32),
            ],
            cost_estimate=cost,
            compiler_params=params,
            name="bwd",
        )(*operands)

    def gate(tick, direct, distant, keep_gproj):
        extra = [value for value in (direct, distant) if value is not None]
        operands = (info, edge_grad, *extra, modulation, keep_gproj)
        return pl.pallas_call(
            functools.partial(
                gate_kernel,
                tick,
                units,
                direct is not None,
                distant is not None,
                sections - 1,
                far - 1,
            ),
            in_specs=[smem] + [vmem] * (len(operands) - 1),
            out_specs=vmem,
            out_shape=slots_of(jnp.bfloat16),
            input_output_aliases={len(operands) - 1: 0},
            cost_estimate=pl.CostEstimate(
                flops=rows * width, bytes_accessed=4 * rows * width, transcendentals=0
            ),
            compiler_params=params,
            name="gate",
        )(*operands)

    def send(value, tick, delays, step, is_far):
        pairs, wanted = [], False
        for s in range(sections):
            to = s + step
            if 0 <= to < sections and ((s < far) != (to < far)) == is_far:
                pairs.append((s, to))
                wanted = wanted or 0 <= tick - delays[s] < units
        return lax.ppermute(value, "section", pairs) if wanted else None

    kept, sofar, join_parts = [], [], []
    near_f, far_f, near_b, far_b = {}, {}, {}, {}
    last = depth + units - 1
    for tick in range(depth + last):
        if tick <= last:
            weights = [value_weight, proj_weight] if tick < JOINS else [joined]
            block_out, *kept = forward(tick, near_f.get(tick), far_f.get(tick), kept, weights)
            if tick < JOINS:
                block_out, value_weight, join_parts = lax.optimization_barrier(
                    (block_out, value_weight, join_parts)
                )
                joined = join(tick, join_parts)
                join_parts = [joined]
            near_f[tick + 1] = send(block_out, tick, delay, 1, False)
            far_f[tick + 2] = send(block_out, tick, delay, 1, True)
        back = tick - depth
        if back >= 0:
            grad_in, *rest = backward(
                back, near_b.get(back), far_b.get(back), kept[0], kept[2], sofar
            )
            sofar = [rest[1], rest[0]]
            if back == last - 4:
                grad_in, keep_mod = lax.optimization_barrier((grad_in, kept[1]))
                tall_val = batch_product(keep_mod, value_weight, False, True)
            if back == last - 5:
                grad_in, keep_mod = lax.optimization_barrier((grad_in, kept[1]))
                tall_mod = in_vmem(
                    turn_kernel, "turn", [bf16_of(width, units * rows)], (keep_mod,), flops=1 << 30
                )[0]
            if back == last - 1:
                grad_in, sofar = lax.optimization_barrier((grad_in, sofar))
                keep_gval = batch_product(sofar[1], proj_weight, True, False)
            near_b[back + 1] = send(grad_in, back, back_delay, -1, False)
            far_b[back + 2] = send(grad_in, back, back_delay, -1, True)

    direct, distant = near_b.get(last), far_b.get(last)
    table, keep_gproj = sofar
    direct, keep_gproj, keep_gval = lax.optimization_barrier((direct, keep_gproj, keep_gval))
    keep_gproj = gate(last, direct, distant, keep_gproj)
    proj_halves = split_product(tall_val, keep_gproj, core)
    right, proj_halves = lax.optimization_barrier((keep_gproj, proj_halves))
    keep_gval = in_vmem(
        functools.partial(value_kernel, last, units),
        "value",
        [slots_of(jnp.bfloat16)],
        (info, right, proj_weight, keep_gval),
        1,
        aliases={3: 0},
        flops=flops,
    )[0]
    value_halves = split_product(tall_mod, keep_gval, core)
    proj_open = opened(proj_halves, outer_turns)
    direct, proj_open = lax.optimization_barrier((direct, proj_open))
    table = backward(
        last, direct, distant, kept[0], kept[2], [table, keep_gproj], final=True
    )[0]
    value_open = opened(value_halves, outer_turns)

    def toward(parts):
        ahead, behind = parts
        return turned(ahead, DP[0], 1), turned(behind, DP[0], -1)

    proj_around = toward(relayed(*proj_open[1:]))
    value_around = toward(relayed(*value_open[1:]))
    proj_divided = divided((proj_open[0], *proj_around), inner_turns)
    proj_parts = sent_around(proj_divided)
    value_around, _ = lax.optimization_barrier((value_around, proj_divided))
    value_divided, table = lax.optimization_barrier(
        (divided((value_open[0], *value_around), inner_turns), table)
    )
    value_parts = sent_around(value_divided)
    table_part = summed_on_arrival(jnp.sum(table, axis=1), DP, 1)
    proj_part = summed(*proj_parts)
    value_part = summed(*value_parts)
    return (value_part[None], proj_part[None], table_part[None])


def solution(mesh):
    finer = Mesh(
        mesh.devices.reshape(mesh.shape["section"], 4, 4, 2), ("section", "dp_0", "dp_1", "dp_2")
    )
    placed = (
        P(None, DP, None),
        P(None, DP, None),
        P(),
        P(),
        P(),
        P("section", None, None),
        P("section", None, None),
        P("section", None, None),
    )
    return jax.shard_map(
        per_device,
        mesh=finer,
        in_specs=placed,
        out_specs=(P("section", DP, None), P("section", DP, None), P("section", None, DP)),
        check_vma=False,
    )
```
